32 devices in a mesh: row: 4 (over y, x), col: 8 (over z, core).
Axes of the slice: x: 2, y: 2, z: 4, core: 2. Of those that a mesh axis runs over, the one named last changes fastest.
Arguments:
- pair: bfloat16 [128, 128, 128], P('row', 'col'), may hold values from -6 to 6
- cotangent: bfloat16 [128, 128, 128], P('row', 'col'), may hold values from -6 to 6
- token_mask: int32 [128], replicated, may hold values 0 or 1
- out_in_proj: bfloat16 [128, 640], replicated, may hold values from -0.5 to 0.5
- out_out_proj: bfloat16 [128, 128], replicated, may hold values from -0.5 to 0.5
- in_in_proj: bfloat16 [128, 640], replicated, may hold values from -0.5 to 0.5
- in_out_proj: bfloat16 [128, 128], replicated, may hold values from -0.5 to 0.5
Outputs:
- updated_pair: bfloat16 [128, 128, 128], P('row', 'col')
- pair_grad: bfloat16 [128, 128, 128], P('row', 'col')
- out_in_grad: float32 [128, 640], replicated
- out_out_grad: float32 [128, 128], replicated
- in_in_grad: float32 [128, 640], replicated
- in_out_grad: float32 [128, 128], replicated
The draws below stay inside these ranges and needn't reach their ends.
All inputs are finite; a program needn't handle non-finite values.
Results may differ from the reference program's by a relative error of at most 0.012.
Values may be sent and summed in bfloat16 or wider, within the bound.
No kernel may reach another device: no remote copies, remote signals or barrier semaphores. Data moves between devices by JAX's collectives and lax.ppermute only.
A program may use at most 128 MiB of HBM per device.

```python
import jax
import jax.numpy as jnp
from jax import lax

C = 128
H = 128
TOKENS = 128


def with_ends(values, stream_key, low, largest):
    longest = values.shape.index(max(values.shape))
    spots = []
    for shift in (0, 1):
        where = [jax.random.randint(jax.random.fold_in(stream_key, axis), (), 0, length) for axis, length in enumerate(values.shape)]
        where[longest] = (where[longest] + shift) % values.shape[longest]
        spots.append(tuple(where))
    return values.at[spots[0]].set(low).at[spots[1]].set(largest)


def shard_levels(own_key, extent, split, least, largest):
    gain, own = 1.0, jax.random.fold_in(own_key, 6)
    for axis_at, blocks in split:
        heights = jnp.exp(jax.random.uniform(jax.random.fold_in(own, axis_at), (blocks,), jnp.float32, least / len(split), largest / len(split)))
        gain = gain * jnp.repeat(heights, extent[axis_at] // blocks).reshape([-1 if axis == axis_at else 1 for axis in range(len(extent))])
    return gain


def centred(rng, extent, scale, reach, shards=(), kind=jnp.bfloat16):
    loudness = shard_levels(rng, extent, shards, -0.22, 0.18) if shards else 1.0
    entries = jax.random.normal(rng, extent, jnp.float32) * scale * loudness
    return jnp.minimum(jnp.maximum(entries, -reach), reach).astype(kind)


def setup_inputs(seed: int = 0) -> dict:
    streams_of = jax.random.split(jax.random.key(seed), 8)
    return {
        "pair": centred(streams_of[0], (TOKENS, TOKENS, C), 1.0, 6.0, ((0, 4), (1, 8))),
        "cotangent": centred(streams_of[1], (TOKENS, TOKENS, C), 1.0, 6.0, ((0, 4), (1, 8))),
        "token_mask": with_ends((jax.random.randint(streams_of[2], (TOKENS,), 0, 8) < 7).astype(jnp.int32), jax.random.fold_in(streams_of[2], 1), 0, 1),
        "out_in_proj": centred(streams_of[3], (C, 4 * H + C), C ** -0.5, 0.5),
        "out_out_proj": centred(streams_of[4], (H, C), H ** -0.5, 0.5),
        "in_in_proj": centred(streams_of[5], (C, 4 * H + C), C ** -0.5, 0.5),
        "in_out_proj": centred(streams_of[6], (H, C), H ** -0.5, 0.5),
    }


EPSILON = 1e-05

def normalize(values):
    centre = lax.optimization_barrier(jnp.mean(values, axis=-1, keepdims=True))
    shifted = values - centre
    spread = lax.optimization_barrier(jnp.mean(shifted * shifted, axis=-1, keepdims=True))
    return shifted * lax.rsqrt(spread + EPSILON)

def gating(projected, pair_mask):
    left_value = projected[..., :H]
    left_gate = projected[..., H:2 * H]
    right_value = projected[..., 2 * H:3 * H]
    right_gate = projected[..., 3 * H:4 * H]
    left_full = jax.nn.sigmoid(left_gate) * left_value * pair_mask
    right_full = jax.nn.sigmoid(right_gate) * right_value * pair_mask
    return (left_full, right_full, jax.nn.sigmoid(projected[..., 4 * H:]))

def triangle(left_tile, right_tile, outgoing):
    left_wide = left_tile.astype(jnp.float32)
    right_wide = right_tile.astype(jnp.float32)
    if outgoing:
        return jnp.einsum('ikh,jkh->ijh', left_wide, right_wide)
    return jnp.einsum('kih,kjh->ijh', left_wide, right_wide)

def triangle_grads(tri_grad, left_tile, right_tile, outgoing):
    grad_wide = tri_grad.astype(jnp.float32)
    left_wide = left_tile.astype(jnp.float32)
    right_wide = right_tile.astype(jnp.float32)
    if outgoing:
        left_grad = jnp.einsum('ijh,jkh->ikh', grad_wide, right_wide)
        right_grad = jnp.einsum('ijh,ikh->jkh', grad_wide, left_wide)
    else:
        left_grad = jnp.einsum('ijh,kjh->kih', grad_wide, right_wide)
        right_grad = jnp.einsum('ijh,kih->kjh', grad_wide, left_wide)
    return (left_grad, right_grad)

def forward(pair_in, pair_mask, w_in, w_out, outgoing):
    pair_wide = pair_in.astype(jnp.float32)
    normed = normalize(pair_wide).astype(jnp.bfloat16)
    projected = jnp.dot(normed, w_in, preferred_element_type=jnp.float32)
    left_full, right_full, gate = gating(projected, pair_mask)
    left_tile = left_full.astype(jnp.bfloat16)
    right_tile = right_full.astype(jnp.bfloat16)
    triangle_sum = triangle(left_tile, right_tile, outgoing)
    tri_normed = normalize(triangle_sum).astype(jnp.bfloat16)
    lifted = jnp.dot(tri_normed, w_out, preferred_element_type=jnp.float32)
    result = (pair_wide + gate * lifted).astype(jnp.bfloat16)
    saved = (pair_wide, normed, projected, left_tile, right_tile, gate, triangle_sum, tri_normed, lifted)
    return (result, saved)

def backward(cotan, saved, pair_mask, w_in, w_out, outgoing):
    pair_wide, normed, projected, left_tile, right_tile, gate, triangle_sum, tri_normed, lifted = saved
    cot_wide = cotan.astype(jnp.float32)
    lift_grad = gate * cot_wide
    gate_grad = lifted * cot_wide
    out_grad = jnp.einsum('ijh,ijc->hc', tri_normed.astype(jnp.float32), lift_grad, precision=lax.Precision.HIGHEST)
    normed_tri_grad = jnp.dot(lift_grad, w_out.astype(jnp.float32).T, precision=lax.Precision.HIGHEST)
    tri_grad = jax.vjp(normalize, triangle_sum)[1](normed_tri_grad)[0].astype(jnp.bfloat16)
    left_grad, right_grad = triangle_grads(tri_grad, left_tile, right_tile, outgoing)
    gate_vjp = jax.vjp(lambda values: gating(values, pair_mask), projected)[1]
    proj_grad = gate_vjp((left_grad, right_grad, gate_grad))[0]
    in_grad = jnp.einsum('ijc,ijq->cq', normed.astype(jnp.float32), proj_grad, precision=lax.Precision.HIGHEST)
    normed_grad = jnp.dot(proj_grad, w_in.astype(jnp.float32).T, precision=lax.Precision.HIGHEST)
    pair_grad = (cot_wide + jax.vjp(normalize, pair_wide)[1](normed_grad)[0]).astype(jnp.bfloat16)
    return (pair_grad, in_grad, out_grad)

def reference(pair, cotangent, token_mask, out_in_proj, out_out_proj, in_in_proj, in_out_proj):
    flags = token_mask.astype(jnp.float32)
    pair_mask = (flags[:, None] * flags[None, :])[:, :, None]
    middle, saved_out = forward(pair, pair_mask, out_in_proj, out_out_proj, True)
    updated, saved_in = forward(middle, pair_mask, in_in_proj, in_out_proj, False)
    middle_grad, in_in_grad, in_out_grad = backward(cotangent, saved_in, pair_mask, in_in_proj, in_out_proj, False)
    pair_grad, out_in_grad, out_out_grad = backward(middle_grad, saved_out, pair_mask, out_in_proj, out_out_proj, True)
    return (updated, pair_grad, out_in_grad / TOKENS, out_out_grad / TOKENS, in_in_grad / TOKENS, in_out_grad / TOKENS)
```

```python
import jax
import jax.numpy as jnp
from jax import lax
from jax.experimental import pallas as pl
from jax.experimental.pallas import tpu as pltpu
from jax.sharding import PartitionSpec as P

EPSILON = 1e-05
LANES = 128
AXES = ("row", "col")
F32 = jnp.float32
BF16 = jnp.bfloat16


class Plan:
    def __init__(self, mesh, tile, width, hidden):
        self.rows = mesh.shape["row"]
        self.cols = mesh.shape["col"]
        self.n = self.rows * self.cols
        self.rt, self.ct = tile
        self.pos = self.rt * self.ct
        self.tokens = self.rt * self.rows
        self.c = width
        self.h = hidden
        self.cpd = hidden // self.n
        self.crow = width // self.n
        self.blocks = LANES // self.rt
        self.lane_groups = self.tokens // LANES
        self.seconds = self.pos // LANES
        assert self.blocks >= 1 and self.cpd == self.crow
        assert self.rt & (self.rt - 1) == 0 and self.rows == self.blocks * self.lane_groups


def nn(a, b):
    return jnp.dot(a, b, preferred_element_type=F32)


def nt(a, b):
    return lax.dot_general(a, b, (((1,), (1,)), ((), ())), preferred_element_type=F32)


def iota(shape, axis):
    return lax.broadcasted_iota(jnp.int32, shape, axis)


def one_hot(cond):
    return jnp.where(cond, 1.0, 0.0).astype(BF16)


def eye(size):
    return one_hot(iota((size, size), 0) == iota((size, size), 1))


def order(plan):
    natural = iota((plan.pos, plan.pos), 0)
    lane = iota((plan.pos, plan.pos), 1)
    shift = plan.rt.bit_length() - 1
    return one_hot(natural == (lane & (plan.rt - 1)) * plan.ct + (lane >> shift))


def to_lanes(tile, plan):
    turned = nt(eye(plan.c), tile).astype(BF16)
    return nn(turned, order(plan))


def from_lanes(lanes, plan):
    return nt(order(plan), lanes).astype(BF16)


def split_order(plan):
    wide = 2 * plan.h
    row = iota((wide, wide), 0)
    source = iota((wide, wide), 1)
    per = 2 * plan.cpd
    bits = per.bit_length() - 1
    side = (row & (per - 1)) >> (bits - 1)
    channel = (row >> bits) * plan.cpd + (row & (plan.cpd - 1))
    return one_hot(source == side * plan.h + channel)


def sides(w, first, plan):
    h = plan.h
    return jnp.concatenate([w[:, first * h : (first + 1) * h], w[:, (first + 2) * h : (first + 3) * h]], axis=1)


def standard(x):
    centre = jnp.mean(x, axis=0, keepdims=True)
    shifted = x - centre
    spread = jnp.mean(shifted * shifted, axis=0, keepdims=True)
    scale = lax.rsqrt(spread + EPSILON)
    return shifted * scale, scale


def standard_grad(unit, scale, grad):
    flat = jnp.mean(grad, axis=0, keepdims=True)
    along = jnp.mean(grad * unit, axis=0, keepdims=True)
    return scale * (grad - flat - unit * along)


def split_projection(normed, w, plan):
    perm = split_order(plan)
    value = nn(nt(perm, sides(w, 0, plan)).astype(BF16), normed)
    gate = jax.nn.sigmoid(nn(nt(perm, sides(w, 1, plan)).astype(BF16), normed))
    return value, gate


def out_gate(normed, w, plan):
    tail = nt(eye(plan.h), w[:, 4 * plan.h :]).astype(BF16)
    return jax.nn.sigmoid(nn(tail, normed))


def lift(tri, w_out, plan):
    unit, scale = standard(tri)
    rounded = unit.astype(BF16)
    lifted = nn(nt(eye(plan.c), w_out).astype(BF16), rounded)
    return unit, scale, rounded, lifted


def put_rows(dest_ref, value, per, plan, start=0):
    size = value.shape[1]
    for d in range(plan.n):
        dest_ref[d, :, start : start + size] = value[per * d : per * (d + 1), :].astype(dest_ref.dtype)


def get_rows(source_ref, scratch_ref, per, plan, start, size):
    for d in range(plan.n):
        scratch_ref[per * d : per * (d + 1), :size] = source_ref[d, :, start : start + size].astype(F32)
    return scratch_ref[:, :size]


def first_kernel(plan):
    def body(idx, pair, tokens, w_in, x_ref, z_ref, mask_ref):
        z = to_lanes(pair[...], plan)
        z_ref[...] = z.astype(BF16)
        token = iota((plan.tokens, plan.pos), 0)
        lane = iota((plan.tokens, plan.pos), 1)
        shift = plan.rt.bit_length() - 1
        first = one_hot(token == idx[0] * plan.rt + (lane & (plan.rt - 1)))
        second = one_hot(token == idx[1] * plan.ct + (lane >> shift))
        flags = jnp.broadcast_to(tokens[...].astype(F32), (8, plan.tokens)).astype(BF16)
        mask = nn(flags, first) * nn(flags, second)
        mask_ref[...] = mask
        normed = standard(z)[0].astype(BF16)
        value, gate = split_projection(normed, w_in[...], plan)
        put_rows(x_ref, gate * value * mask[:1], 2 * plan.cpd, plan)

    return body


def middle_kernel(plan):
    def body(z_ref, y_ref, mask_ref, w_in1, w_out1, w_in2, x_ref, mid_ref, scr):
        z = z_ref[...].astype(F32)
        normed = standard(z)[0].astype(BF16)
        gate = out_gate(normed, w_in1[...], plan)
        tri = get_rows(y_ref, scr, plan.cpd, plan, 0, plan.pos)
        lifted = lift(tri, w_out1[...], plan)[3]
        mid = (z + gate * lifted).astype(BF16)
        mid_ref[...] = mid
        normed = standard(mid.astype(F32))[0].astype(BF16)
        value, side_gate = split_projection(normed, w_in2[...], plan)
        put_rows(x_ref, side_gate * value * mask_ref[:1, :], 2 * plan.cpd, plan)

    return body


def lift_backward(dres, gate, tri, w_out, plan):
    unit, scale, rounded, lifted = lift(tri, w_out, plan)
    lift_grad = (gate * dres).astype(BF16)
    gate_grad = lifted * dres * gate * (1.0 - gate)
    out_grad = nt(rounded, lift_grad)
    tri_grad = standard_grad(unit, scale, nn(w_out, lift_grad))
    return lifted, gate_grad.astype(BF16), out_grad, tri_grad


def turn_kernel(plan):
    def body(mid_ref, y_ref, cot_ref, w_in2, w_out2, up_ref, x_ref, cot_out, dog_ref, og_ref, scr):
        mid = mid_ref[...].astype(F32)
        cot = to_lanes(cot_ref[...], plan)
        cot_out[...] = cot.astype(BF16)
        normed = standard(mid)[0].astype(BF16)
        gate = out_gate(normed, w_in2[...], plan)
        tri = get_rows(y_ref, scr, plan.cpd, plan, 0, plan.pos)
        lifted, dog, out_grad, tri_grad = lift_backward(cot, gate, tri, w_out2[...], plan)
        up_ref[...] = from_lanes((mid + gate * lifted).astype(BF16), plan)
        dog_ref[...] = dog
        og_ref[...] = out_grad
        put_rows(x_ref, tri_grad, plan.cpd, plan)

    return body


def input_backward(source, sides_grad, dog, mask, w, plan):
    unit, scale = standard(source)
    normed = unit.astype(BF16)
    value, gate = split_projection(normed, w, plan)
    through = sides_grad * mask * gate
    value_grad = through.astype(BF16)
    gate_grad = (through * value * (1.0 - gate)).astype(BF16)
    perm = split_order(plan)
    value_w = nt(sides(w, 0, plan), perm).astype(BF16)
    gate_w = nt(sides(w, 1, plan), perm).astype(BF16)
    normed_grad = nn(value_w, value_grad) + nn(gate_w, gate_grad) + nn(w[:, 4 * plan.h :], dog)
    value_part = nn(nt(normed, value_grad).astype(BF16), perm)
    gate_part = nn(nt(normed, gate_grad).astype(BF16), perm)
    h = plan.h
    parts = [value_part[:, :h], gate_part[:, :h], value_part[:, h:], gate_part[:, h:]]
    return standard_grad(unit, scale, normed_grad), parts, normed


def back_kernel(plan):
    def body(mid_ref, y6, cot_ref, dog2, og2, mask_ref, w_in2, z_ref, y2, w_in1, w_out1,
             x_ref, mg_ref, dog1_ref, scr, scr2):
        cot = cot_ref[...].astype(F32)
        sides_grad = get_rows(y6, scr2, 2 * plan.cpd, plan, 0, plan.pos)
        term, parts, normed = input_backward(
            mid_ref[...].astype(F32), sides_grad, dog2[...], mask_ref[:1, :], w_in2[...], plan
        )
        gate_part = nt(normed, dog2[...])
        mid_grad = (cot + term).astype(BF16)
        mg_ref[...] = mid_grad
        normed1 = standard(z_ref[...].astype(F32))[0].astype(BF16)
        gate = out_gate(normed1, w_in1[...], plan)
        tri = get_rows(y2, scr, plan.cpd, plan, 0, plan.pos)
        _, dog, out_grad, tri_grad = lift_backward(mid_grad.astype(F32), gate, tri, w_out1[...], plan)
        dog1_ref[...] = dog
        put_rows(x_ref, tri_grad, plan.cpd, plan)
        terms = parts + [gate_part, og2[...], out_grad, nt(normed1, dog)]
        at = plan.pos
        for part in terms:
            put_rows(x_ref, part, plan.crow, plan, at)
            at += part.shape[1]

    return body


def last_kernel(plan):
    def body(y8, z_ref, mg_ref, dog_ref, mask_ref, w_in1, x_ref, pg_ref, in2_ref, out2_ref, out1_ref, g1_ref, scr2):
        h, crow = plan.h, plan.crow
        sides_grad = get_rows(y8, scr2, 2 * plan.cpd, plan, 0, plan.pos)
        term, parts, _ = input_backward(
            z_ref[...].astype(F32), sides_grad, dog_ref[...], mask_ref[:1, :], w_in1[...], plan
        )
        pg_ref[...] = from_lanes((mg_ref[...].astype(F32) + term).astype(BF16), plan)
        at = 0
        for part in parts:
            put_rows(x_ref, part, crow, plan, at)
            at += h
        half = 4 * h
        for d in range(plan.n):
            low = y8[d, :crow, plan.pos :].astype(F32)
            high = y8[d, crow : 2 * crow, plan.pos :].astype(F32)
            rows = slice(crow * d, crow * (d + 1))
            in2_ref[rows, :half] = low
            in2_ref[rows, half:] = high[:, :h]
            out2_ref[rows, :] = high[:, h : 2 * h]
            out1_ref[rows, :] = high[:, 2 * h : 3 * h]
            g1_ref[rows, :] = high[:, 3 * h :]

    return body


def sum_kernel(plan):
    def body(y_ref, x_ref):
        total = y_ref[0].astype(F32)
        for d in range(1, plan.n):
            total = total + y_ref[d].astype(F32)
        total = (total * (1.0 / plan.tokens)).astype(BF16)
        for d in range(plan.n):
            x_ref[d] = total

    return body


def end_kernel(plan):
    def body(y_ref, g1_ref, out_ref):
        width = 4 * plan.h
        for d in range(plan.n):
            out_ref[plan.crow * d : plan.crow * (d + 1), :width] = y_ref[d].astype(F32)
        out_ref[:, width:] = g1_ref[...]

    return body


def turn_blocks(group, plan):
    count, size = plan.blocks, plan.rt
    lane = iota(group[0].shape, 1)
    group = list(group)
    step = count // 2
    while step:
        low = (lane & (step * size)) == 0
        for a in range(count):
            if a & step == 0:
                x, y = group[a], group[a + step]
                group[a] = jnp.where(low, x, pltpu.roll(y, step * size, 1))
                group[a + step] = jnp.where(low, pltpu.roll(x, LANES - step * size, 1), y)
        step //= 2
    return group


def spread(y_ref, scr, per, plan):
    for c in range(plan.cols):
        for g in range(plan.lane_groups):
            for q in range(plan.seconds):
                group = []
                for b in range(plan.blocks):
                    src = (g * plan.blocks + b) * plan.cols + c
                    group.append(y_ref[src, :per, q * LANES : (q + 1) * LANES].astype(F32))
                group = turn_blocks(group, plan)
                for b in range(plan.blocks):
                    second = c * plan.ct + q * plan.blocks + b
                    scr[g, second * per : (second + 1) * per, :] = group[b]


def collect(scr, x_ref, per, plan):
    for c in range(plan.cols):
        for g in range(plan.lane_groups):
            for q in range(plan.seconds):
                group = []
                for b in range(plan.blocks):
                    second = c * plan.ct + q * plan.blocks + b
                    group.append(scr[g, second * per : (second + 1) * per, :])
                group = turn_blocks(group, plan)
                for b in range(plan.blocks):
                    dest = (g * plan.blocks + b) * plan.cols + c
                    x_ref[dest, :per, q * LANES : (q + 1) * LANES] = group[b].astype(BF16)


def pick(scr, row, per, plan):
    parts = [scr[g, pl.ds(row, plan.tokens, stride=per), :] for g in range(plan.lane_groups)]
    return parts[0] if len(parts) == 1 else jnp.concatenate(parts, axis=1)


def place(scr, row, per, value, plan):
    for g in range(plan.lane_groups):
        scr[g, pl.ds(row, plan.tokens, stride=per), :] = value[:, g * LANES : (g + 1) * LANES]


def product_kernel(plan, outgoing):
    cpd = plan.cpd

    def body(y_ref, x_ref, lr_ref, scr, scr_out):
        spread(y_ref, scr, 2 * cpd, plan)
        for t in range(cpd):
            left = pick(scr, t, 2 * cpd, plan)
            right = pick(scr, cpd + t, 2 * cpd, plan)
            left_b, right_b = left.astype(BF16), right.astype(BF16)
            lr_ref[t] = left_b
            lr_ref[cpd + t] = right_b
            tri = nn(right.T.astype(BF16), left_b) if outgoing else nt(right_b, left_b)
            place(scr_out, t, cpd, tri, plan)
        collect(scr_out, x_ref, cpd, plan)

    return body


def grad_kernel(plan, outgoing, width):
    cpd = plan.cpd

    def body(y_ref, lr_ref, x_ref, scr, scr_out):
        spread(y_ref, scr, cpd, plan)
        for t in range(cpd):
            grad = pick(scr, t, cpd, plan)
            grad_b = grad.astype(BF16)
            left, right = lr_ref[t], lr_ref[cpd + t]
            if outgoing:
                left_grad, right_grad = nn(right, grad_b), nt(left, grad_b)
            else:
                left_grad, right_grad = nn(grad.T.astype(BF16), right), nn(grad_b, left)
            place(scr_out, t, 2 * cpd, left_grad, plan)
            place(scr_out, cpd + t, 2 * cpd, right_grad, plan)
        collect(scr_out, x_ref, 2 * cpd, plan)
        if width:
            total = y_ref[0, :, plan.pos :].astype(F32)
            for d in range(1, plan.n):
                total = total + y_ref[d, :, plan.pos :].astype(F32)
            total = (total * (1.0 / plan.tokens)).astype(BF16)
            half = width // 2
            for d in range(plan.n):
                x_ref[d, :cpd, plan.pos :] = total[:, :half]
                x_ref[d, cpd : 2 * cpd, plan.pos :] = total[:, half:]

    return body


def call(body, name, outs, args, scratch=(), scalars=0):
    whole = pl.BlockSpec(memory_space=pltpu.VMEM)
    return pl.pallas_call(
        body,
        name=name,
        in_specs=[pl.BlockSpec(memory_space=pltpu.SMEM)] * scalars + [whole] * (len(args) - scalars),
        out_specs=[whole] * len(outs),
        out_shape=[jax.ShapeDtypeStruct(shape, kind) for shape, kind in outs],
        scratch_shapes=[pltpu.VMEM(shape, F32) for shape in scratch],
        compiler_params=pltpu.CompilerParams(vmem_limit_bytes=48 * 1024 * 1024),
    )(*args)


def exchange(x):
    return lax.all_to_all(x, AXES, 0, 0)


def solution(mesh):
    def local(pair, cotangent, token_mask, w_in1, w_out1, w_in2, w_out2):
        rt, ct, c = pair.shape
        h = w_out1.shape[0]
        plan = Plan(mesh, (rt, ct), c, h)
        n, cpd, pos, tokens = plan.n, plan.cpd, plan.pos, plan.tokens
        idx = jnp.stack([lax.axis_index("row"), lax.axis_index("col")]).astype(jnp.int32)
        lanes = (c, pos)
        both = (n, 2 * cpd, pos)
        single = (n, cpd, pos)
        extra = 8 * h
        group = plan.lane_groups
        scr1 = (group, tokens * cpd, LANES)
        scr2 = (group, tokens * 2 * cpd, LANES)

        x1, z, mask = call(
            first_kernel(plan), "first", [(both, BF16), (lanes, BF16), ((8, pos), F32)],
            [idx, pair.reshape(pos, c), token_mask.reshape(1, tokens), w_in1], scalars=1,
        )
        y1 = exchange(x1)
        x2, lr1 = call(
            product_kernel(plan, True), "product_out", [(single, BF16), ((2 * cpd, tokens, tokens), BF16)],
            [y1], [scr2, scr1],
        )
        y2 = exchange(x2)
        x3, mid = call(
            middle_kernel(plan), "middle", [(both, BF16), (lanes, BF16)],
            [z, y2, mask, w_in1, w_out1, w_in2], [(h, pos)],
        )
        y3 = exchange(x3)
        x4, lr2 = call(
            product_kernel(plan, False), "product_in", [(single, BF16), ((2 * cpd, tokens, tokens), BF16)],
            [y3], [scr2, scr1],
        )
        y4 = exchange(x4)
        updated, x5, cot, dog2, og2 = call(
            turn_kernel(plan), "turn",
            [((pos, c), BF16), (single, BF16), (lanes, BF16), (lanes, BF16), ((h, c), F32)],
            [mid, y4, cotangent.reshape(pos, c), w_in2, w_out2], [(h, pos)],
        )
        y5 = exchange(x5)
        (x6,) = call(grad_kernel(plan, False, 0), "grads_in", [(both, BF16)], [y5, lr2], [scr1, scr2])
        y6 = exchange(x6)
        x7, mid_grad, dog1 = call(
            back_kernel(plan), "back", [((n, cpd, pos + extra), BF16), (lanes, BF16), (lanes, BF16)],
            [mid, y6, cot, dog2, og2, mask, w_in2, z, y2, w_in1, w_out1], [(h, pos), (2 * h, pos)],
        )
        y7 = exchange(x7)
        (x8,) = call(
            grad_kernel(plan, True, extra), "grads_out", [((n, 2 * cpd, pos + extra // 2), BF16)],
            [y7, lr1], [scr1, scr2],
        )
        y8 = exchange(x8)
        x9, pair_grad, in2, out2, out1, g1 = call(
            last_kernel(plan), "last",
            [((n, cpd, 4 * h), BF16), ((pos, c), BF16), ((c, 5 * h), F32), ((h, c), F32), ((h, c), F32), ((c, h), F32)],
            [y8, z, mid_grad, dog1, mask, w_in1], [(2 * h, pos)],
        )
        y9 = exchange(x9)
        (x10,) = call(sum_kernel(plan), "sum", [((n, cpd, 4 * h), BF16)], [y9])
        y10 = exchange(x10)
        (in1,) = call(end_kernel(plan), "end", [((c, 5 * h), F32)], [y10, g1])
        return updated.reshape(rt, ct, c), pair_grad.reshape(rt, ct, c), in1, out1, in2, out2

    return jax.shard_map(
        local,
        mesh=mesh,
        in_specs=(P("row", "col", None), P("row", "col", None), P(), P(), P(), P(), P()),
        out_specs=(P("row", "col", None), P("row", "col", None), P(), P(), P(), P()),
        check_vma=False,
    )
```

```python
import jax
import jax.numpy as jnp
from jax import lax
from jax.experimental import pallas as pl
from jax.experimental.pallas import tpu as pltpu
from jax.sharding import PartitionSpec as P

EPSILON = 1e-05
LANES = 128
AXES = ("row", "col")
F32 = jnp.float32
BF16 = jnp.bfloat16


class Plan:
    def __init__(self, mesh, tile, width, hidden):
        self.rows = mesh.shape["row"]
        self.cols = mesh.shape["col"]
        self.n = self.rows * self.cols
        self.rt, self.ct = tile
        self.pos = self.rt * self.ct
        self.tokens = self.rt * self.rows
        self.c = width
        self.h = hidden
        self.cpd = hidden // self.n
        self.crow = width // self.n
        self.blocks = LANES // self.rt
        self.lane_groups = self.tokens // LANES
        self.seconds = self.pos // LANES
        self.wide = 8 * hidden // self.n * (width // 2) // (2 * self.crow)
        assert self.blocks >= 1 and self.cpd == self.crow
        assert self.rt & (self.rt - 1) == 0 and self.rows == self.blocks * self.lane_groups


def nn(a, b):
    return jnp.dot(a, b, preferred_element_type=F32)


def nt(a, b):
    return lax.dot_general(a, b, (((1,), (1,)), ((), ())), preferred_element_type=F32)


def iota(shape, axis):
    return lax.broadcasted_iota(jnp.int32, shape, axis)


def one_hot(cond):
    return jnp.where(cond, 1.0, 0.0).astype(BF16)


def eye(size):
    return one_hot(iota((size, size), 0) == iota((size, size), 1))


def to_lanes(tile_ref, scr, plan):
    scr[...] = tile_ref[...].astype(F32)
    rows = [scr[pl.ds(k, plan.rt, stride=plan.ct), :] for k in range(plan.ct)]
    return nt(eye(plan.c), jnp.concatenate(rows, axis=0).astype(BF16))


def from_lanes(lanes, scr, plan):
    turn = eye(LANES)
    for q in range(plan.seconds):
        block = nt(turn, lanes[:, q * LANES : (q + 1) * LANES])
        for b in range(plan.blocks):
            rows = block[b * plan.rt : (b + 1) * plan.rt, :]
            scr[pl.ds(q * plan.blocks + b, plan.rt, stride=plan.ct), :] = rows
    return scr[...].astype(BF16)


def split_order(plan):
    wide = 2 * plan.h
    row = iota((wide, wide), 0)
    source = iota((wide, wide), 1)
    per = 2 * plan.cpd
    bits = per.bit_length() - 1
    side = (row & (per - 1)) >> (bits - 1)
    channel = (row >> bits) * plan.cpd + (row & (plan.cpd - 1))
    return one_hot(source == side * plan.h + channel)


def sides(w, first, plan):
    h = plan.h
    return jnp.concatenate([w[:, first * h : (first + 1) * h], w[:, (first + 2) * h : (first + 3) * h]], axis=1)


def standard(x):
    centre = jnp.mean(x, axis=0, keepdims=True)
    shifted = x - centre
    spread = jnp.mean(shifted * shifted, axis=0, keepdims=True)
    scale = lax.rsqrt(spread + EPSILON)
    return shifted * scale, scale


def standard_grad(unit, scale, grad):
    flat = jnp.mean(grad, axis=0, keepdims=True)
    along = jnp.mean(grad * unit, axis=0, keepdims=True)
    return scale * (grad - flat - unit * along)


def split_weights(w, plan):
    perm = split_order(plan)
    return nt(perm, sides(w, 0, plan)).astype(BF16), nt(perm, sides(w, 1, plan)).astype(BF16)


def split_projection(normed, value_w, gate_w):
    return nn(value_w, normed), jax.nn.sigmoid(nn(gate_w, normed))


def out_gate(normed, w, plan):
    tail = nt(eye(plan.h), w[:, 4 * plan.h :]).astype(BF16)
    return jax.nn.sigmoid(nn(tail, normed))


def back_coefficients(normed, w, mask, plan):
    value, gate = split_projection(normed, *split_weights(w, plan))
    through = gate * mask
    return through, through * value * (1.0 - gate)


def back_weights(w, plan):
    perm = split_order(plan)
    return nt(sides(w, 0, plan), perm).astype(BF16), nt(sides(w, 1, plan), perm).astype(BF16)


def side_terms(normed, value_grad, gate_grad, plan):
    perm = split_order(plan)
    value_part = nn(nt(normed, value_grad).astype(BF16), perm)
    gate_part = nn(nt(normed, gate_grad).astype(BF16), perm)
    h = plan.h
    return [value_part[:, :h], gate_part[:, :h], value_part[:, h:], gate_part[:, h:]]


def put_rows(dest_ref, value, per, plan, start=0):
    size = value.shape[1]
    for d in range(plan.n):
        dest_ref[d, :, start : start + size] = value[per * d : per * (d + 1), :].astype(dest_ref.dtype)


def get_rows(source_ref, scratch_ref, per, plan, start, size):
    for d in range(plan.n):
        scratch_ref[per * d : per * (d + 1), :size] = source_ref[d, :, start : start + size].astype(F32)
    return scratch_ref[:, :size]


def first_kernel(plan):
    def body(idx, pair_hbm, tokens_hbm, w_hbm, x_ref, z_ref, mask_ref, pair, tokens, w_in, scr, sems):
        sources = (pair_hbm, tokens_hbm, w_hbm)
        copies = [
            pltpu.make_async_copy(source, dest, sems.at[i])
            for i, (source, dest) in enumerate(zip(sources, (pair, tokens, w_in)))
        ]
        for copy in copies:
            copy.start()
        token = iota((plan.tokens, plan.pos), 0)
        lane = iota((plan.tokens, plan.pos), 1)
        shift = plan.rt.bit_length() - 1
        first = one_hot(token == idx[0] * plan.rt + (lane & (plan.rt - 1)))
        second = one_hot(token == idx[1] * plan.ct + (lane >> shift))
        copies[1].wait()
        flags = jnp.broadcast_to(tokens[...].astype(F32), (8, plan.tokens)).astype(BF16)
        mask = nn(flags, first) * nn(flags, second)
        mask_ref[...] = mask
        copies[0].wait()
        z = to_lanes(pair, scr, plan)
        z_ref[...] = z.astype(BF16)
        normed = standard(z)[0].astype(BF16)
        copies[2].wait()
        value, gate = split_projection(normed, *split_weights(w_in[...], plan))
        put_rows(x_ref, gate * value * mask[:1], 2 * plan.cpd, plan)

    return body


def middle_kernel(plan):
    def body(z_ref, y_ref, mask_ref, w_in1, w_out1, w_in2, x_ref, mid_ref, scr):
        z = z_ref[...].astype(F32)
        gate = out_gate(standard(z)[0].astype(BF16), w_in1[...], plan)
        tri = get_rows(y_ref, scr, plan.cpd, plan, 0, plan.pos)
        lifted = nn(nt(eye(plan.c), w_out1[...]).astype(BF16), standard(tri)[0].astype(BF16))
        mid = (z + gate * lifted).astype(BF16)
        mid_ref[...] = mid
        normed = standard(mid.astype(F32))[0].astype(BF16)
        value, gate = split_projection(normed, *split_weights(w_in2[...], plan))
        put_rows(x_ref, gate * value * mask_ref[:1, :], 2 * plan.cpd, plan)

    return body


def turn_kernel(plan):
    def body(y_ref, mid_ref, cot_ref, w_in2, w_out2, x_ref, cot_out, scr, flat):
        cot = to_lanes(cot_ref, flat, plan)
        cot_out[...] = cot.astype(BF16)
        gate = out_gate(standard(mid_ref[...].astype(F32))[0].astype(BF16), w_in2[...], plan)
        lift_grad = (gate * cot).astype(BF16)
        unit, scale = standard(get_rows(y_ref, scr, plan.cpd, plan, 0, plan.pos))
        put_rows(x_ref, standard_grad(unit, scale, nn(w_out2[...], lift_grad)), plan.cpd, plan)

    return body


def after_turn_kernel(plan):
    def body(after, y_ref, mid_ref, cot_ref, w_in2, w_out2, up_hbm, dog_ref, og_ref, gg_ref, scr, flat, up, sem):
        tri = get_rows(y_ref, scr, plan.cpd, plan, 0, plan.pos)
        rounded = standard(tri)[0].astype(BF16)
        lifted = nn(nt(eye(plan.c), w_out2[...]).astype(BF16), rounded)
        mid, cot = mid_ref[...].astype(F32), cot_ref[...].astype(F32)
        normed = standard(mid)[0].astype(BF16)
        gate = out_gate(normed, w_in2[...], plan)
        up[...] = from_lanes((mid + gate * lifted).astype(BF16), flat, plan)
        copy = pltpu.make_async_copy(up, up_hbm, sem)
        copy.start()
        dog = (lifted * cot * gate * (1.0 - gate)).astype(BF16)
        dog_ref[...] = dog
        og_ref[...] = nt(rounded, (gate * cot).astype(BF16))
        gg_ref[...] = nt(normed, dog)
        copy.wait()

    return body


def before_back_kernel(plan):
    def body(after, source_ref, mask_ref, w_in, vc_ref, gc_ref, vw_ref, gw_ref):
        normed = standard(source_ref[...].astype(F32))[0].astype(BF16)
        value, gate = back_coefficients(normed, w_in[...], mask_ref[:1, :], plan)
        vc_ref[...] = value.astype(BF16)
        gc_ref[...] = gate.astype(BF16)
        vw_ref[...], gw_ref[...] = back_weights(w_in[...], plan)

    return body


def gate_kernel(plan):
    def body(after, z_ref, w_in, gate_ref):
        gate_ref[...] = out_gate(standard(z_ref[...].astype(F32))[0].astype(BF16), w_in[...], plan)

    return body


def side_grads(y_ref, vc_ref, gc_ref, scr, plan):
    grad = get_rows(y_ref, scr, 2 * plan.cpd, plan, 0, plan.pos)
    return (grad * vc_ref[...].astype(F32)).astype(BF16), (grad * gc_ref[...].astype(F32)).astype(BF16)


def back_kernel(plan):
    def body(y6, vc_ref, gc_ref, vw_ref, gw_ref, dog_ref, mid_ref, cot_ref, gate_ref, w_in2, w_out1, y2,
             x_ref, mg_ref, scr, scr2):
        value_grad, gate_grad = side_grads(y6, vc_ref, gc_ref, scr2, plan)
        normed_grad = nn(vw_ref[...], value_grad) + nn(gw_ref[...], gate_grad)
        normed_grad += nn(w_in2[:, 4 * plan.h :], dog_ref[...])
        unit, scale = standard(mid_ref[...].astype(F32))
        mid_grad = (cot_ref[...].astype(F32) + standard_grad(unit, scale, normed_grad)).astype(BF16)
        mg_ref[...] = mid_grad
        lift_grad = (gate_ref[...] * mid_grad.astype(F32)).astype(BF16)
        unit, scale = standard(get_rows(y2, scr, plan.cpd, plan, 0, plan.pos))
        put_rows(x_ref, standard_grad(unit, scale, nn(w_out1[...], lift_grad)), plan.cpd, plan)

    return body


def after_back_kernel(plan):
    def body(idx, y6, vc_ref, gc_ref, mid_ref, mg_ref, gate_ref, y2, z_ref, og2, gg2, w_out1,
             keep_ref, send_ref, dog_ref, scr, scr2, sums):
        value_grad, gate_grad = side_grads(y6, vc_ref, gc_ref, scr2, plan)
        terms = side_terms(standard(mid_ref[...].astype(F32))[0].astype(BF16), value_grad, gate_grad, plan)
        mid_grad, gate = mg_ref[...].astype(F32), gate_ref[...]
        lift_grad = (gate * mid_grad).astype(BF16)
        rounded = standard(get_rows(y2, scr, plan.cpd, plan, 0, plan.pos))[0].astype(BF16)
        lifted = nn(nt(eye(plan.c), w_out1[...]).astype(BF16), rounded)
        dog = (lifted * mid_grad * gate * (1.0 - gate)).astype(BF16)
        dog_ref[...] = dog
        normed = standard(z_ref[...].astype(F32))[0].astype(BF16)
        terms += [gg2[...], og2[...], nt(rounded, lift_grad), nt(normed, dog)]
        at = 0
        for part in terms:
            sums[:, at : at + part.shape[1]] = part
            at += part.shape[1]
        half = plan.c // 2
        core = idx[1] & 1
        keep_ref[...] = sums[pl.ds(pl.multiple_of(core * half, 8), half), :]
        send_ref[...] = sums[pl.ds(pl.multiple_of((1 - core) * half, 8), half), :].astype(BF16)

    return body


def last_kernel(plan):
    def body(y8, z_ref, vc_ref, gc_ref, x_ref, scr):
        crow, wide = plan.crow, plan.wide
        value_grad, gate_grad = side_grads(y8, vc_ref, gc_ref, scr, plan)
        normed = standard(z_ref[...].astype(F32))[0].astype(BF16)
        at = 0
        for part in side_terms(normed, value_grad, gate_grad, plan):
            put_rows(x_ref, part, crow, plan, at)
            at += part.shape[1]
        for core in range(2):
            total = y8[core, :, plan.pos :].astype(F32)
            for d in range(core + 2, plan.n, 2):
                total = total + y8[d, :, plan.pos :].astype(F32)
            total = (total * (1.0 / plan.tokens)).astype(BF16)
            for d in range(core, plan.n, 2):
                x_ref[d, :, at : at + wide] = total[:crow, :]
                x_ref[d, :, at + wide :] = total[crow:, :]

    return body


def after_last_kernel(plan):
    def body(after, y8, z_ref, mg_ref, dog_ref, vc_ref, gc_ref, vw_ref, gw_ref, w_in1, pg_hbm, scr, flat, pg, sem):
        value_grad, gate_grad = side_grads(y8, vc_ref, gc_ref, scr, plan)
        normed_grad = nn(vw_ref[...], value_grad) + nn(gw_ref[...], gate_grad)
        normed_grad += nn(w_in1[:, 4 * plan.h :], dog_ref[...])
        unit, scale = standard(z_ref[...].astype(F32))
        grad = mg_ref[...].astype(F32) + standard_grad(unit, scale, normed_grad)
        pg[...] = from_lanes(grad.astype(BF16), flat, plan)
        copy = pltpu.make_async_copy(pg, pg_hbm, sem)
        copy.start()
        copy.wait()

    return body


def sum_kernel(plan):
    def body(y_ref, x_ref):
        width = 4 * plan.h
        total = y_ref[0, :, :width].astype(F32)
        for d in range(1, plan.n):
            total = total + y_ref[d, :, :width].astype(F32)
        total = (total * (1.0 / plan.tokens)).astype(BF16)
        for d in range(plan.n):
            x_ref[d] = total

    return body


def half_kernel(plan):
    def body(y_ref, half_ref):
        half_ref[...] = y_ref[:, :, 4 * plan.h :]

    return body


def assemble_kernel(plan):
    def body(idx, own_ref, other_ref, g1_ref, out1_ref, in2_ref, out2_ref, scr):
        h, crow, wide = plan.h, plan.crow, plan.wide
        half = plan.c // 2
        steps = 8 * h // wide
        per = 2 * crow
        outs = ((in2_ref, 5 * h), (out2_ref, h), (out1_ref, h), (g1_ref, h))
        for k, ref in enumerate((own_ref, other_ref)):
            for d in range(plan.n):
                for g in range(wide // LANES):
                    scr[g, per * d : per * d + crow, :] = ref[d, :, g * LANES : (g + 1) * LANES].astype(F32)
                    scr[g, per * d + crow : per * (d + 1), :] = ref[
                        d, :, wide + g * LANES : wide + (g + 1) * LANES
                    ].astype(F32)
            core = idx[1] & 1 if k == 0 else 1 - (idx[1] & 1)
            rows = pl.ds(pl.multiple_of(core * half, 8), half)
            pieces = [
                scr[g, pl.ds(v, half, stride=steps), :] for v in range(steps) for g in range(wide // LANES)
            ]
            for out_ref, size in outs:
                for i in range(size // LANES):
                    out_ref[rows, i * LANES : (i + 1) * LANES] = pieces.pop(0)

    return body


def end_kernel(plan):
    def body(y_ref, g1_ref, in1_ref):
        crow, width = plan.crow, 4 * plan.h
        for d in range(plan.n):
            in1_ref[crow * d : crow * (d + 1), :width] = y_ref[d].astype(F32)
        in1_ref[:, width:] = g1_ref[...]

    return body


def turn_blocks(group, plan):
    count, size = plan.blocks, plan.rt
    lane = iota(group[0].shape, 1)
    group = list(group)
    step = count // 2
    while step:
        low = (lane & (step * size)) == 0
        for a in range(count):
            if a & step == 0:
                x, y = group[a], group[a + step]
                group[a] = jnp.where(low, x, pltpu.roll(y, step * size, 1))
                group[a + step] = jnp.where(low, pltpu.roll(x, LANES - step * size, 1), y)
        step //= 2
    return group


def spread(y_ref, scr, per, plan):
    for c in range(plan.cols):
        for g in range(plan.lane_groups):
            for q in range(plan.seconds):
                group = []
                for b in range(plan.blocks):
                    src = (g * plan.blocks + b) * plan.cols + c
                    group.append(y_ref[src, :per, q * LANES : (q + 1) * LANES].astype(F32))
                group = turn_blocks(group, plan)
                for b in range(plan.blocks):
                    second = c * plan.ct + q * plan.blocks + b
                    scr[g, second * per : (second + 1) * per, :] = group[b]


def collect(scr, x_ref, per, plan):
    for c in range(plan.cols):
        for g in range(plan.lane_groups):
            for q in range(plan.seconds):
                group = []
                for b in range(plan.blocks):
                    second = c * plan.ct + q * plan.blocks + b
                    group.append(scr[g, second * per : (second + 1) * per, :])
                group = turn_blocks(group, plan)
                for b in range(plan.blocks):
                    dest = (g * plan.blocks + b) * plan.cols + c
                    x_ref[dest, :per, q * LANES : (q + 1) * LANES] = group[b].astype(BF16)


def pick(scr, row, per, plan):
    parts = [scr[g, pl.ds(row, plan.tokens, stride=per), :] for g in range(plan.lane_groups)]
    return parts[0] if len(parts) == 1 else jnp.concatenate(parts, axis=1)


def place(scr, row, per, value, plan):
    for g in range(plan.lane_groups):
        scr[g, pl.ds(row, plan.tokens, stride=per), :] = value[:, g * LANES : (g + 1) * LANES]


def product_kernel(plan, outgoing):
    cpd = plan.cpd

    def body(y_ref, x_ref, lr_ref, scr, scr_out):
        turn = eye(plan.tokens)
        spread(y_ref, scr, 2 * cpd, plan)
        for t in range(cpd):
            left_b = pick(scr, t, 2 * cpd, plan).astype(BF16)
            right_b = pick(scr, cpd + t, 2 * cpd, plan).astype(BF16)
            lr_ref[t] = left_b
            lr_ref[cpd + t] = right_b
            tri = nn(nt(turn, right_b).astype(BF16), left_b) if outgoing else nt(right_b, left_b)
            place(scr_out, t, cpd, tri, plan)
        collect(scr_out, x_ref, cpd, plan)

    return body


def grad_kernel(plan, outgoing):
    cpd = plan.cpd

    def body(*refs):
        if outgoing:
            after, y_ref, lr_ref, keep_ref, other_ref, x_ref, scr, scr_out, scr_sum = refs
        else:
            y_ref, lr_ref, x_ref, scr, scr_out = refs
        turn = eye(plan.tokens)
        spread(y_ref, scr, cpd, plan)
        for t in range(cpd):
            grad_b = pick(scr, t, cpd, plan).astype(BF16)
            left, right = lr_ref[t], lr_ref[cpd + t]
            if outgoing:
                left_grad, right_grad = nn(right, grad_b), nt(left, grad_b)
            else:
                left_grad, right_grad = nn(nt(turn, grad_b).astype(BF16), right), nn(grad_b, left)
            place(scr_out, t, 2 * cpd, left_grad, plan)
            place(scr_out, cpd + t, 2 * cpd, right_grad, plan)
        collect(scr_out, x_ref, 2 * cpd, plan)
        if outgoing:
            half, wide, per = plan.c // 2, plan.wide, 2 * plan.crow
            steps = 8 * plan.h // wide
            total = keep_ref[...] + other_ref[...].astype(F32)
            for v in range(steps):
                for g in range(wide // LANES):
                    at = v * wide + g * LANES
                    scr_sum[g, pl.ds(v, half, stride=steps), :] = total[:, at : at + LANES]
            for d in range(plan.n):
                for g in range(wide // LANES):
                    at = plan.pos + g * LANES
                    x_ref[d, :, at : at + LANES] = scr_sum[g, per * d : per * (d + 1), :].astype(BF16)

    return body


def call(body, name, outs, args, scratch=(), scalars=0, far_in=0, after=0, far_out=()):
    near = pl.BlockSpec(memory_space=pltpu.VMEM)
    far = pl.BlockSpec(memory_space=pltpu.HBM)
    ins = [pl.BlockSpec(memory_space=pltpu.SMEM)] * scalars + [far] * far_in
    args = [
        pltpu.with_memory_space_constraint(a, pltpu.HBM) if scalars <= i < len(ins) else a for i, a in enumerate(args)
    ]
    ins += [pl.BlockSpec(memory_space=pl.ANY)] * after
    return pl.pallas_call(
        body,
        name=name,
        in_specs=ins + [near] * (len(args) - len(ins)),
        out_specs=[far if i in far_out else near for i in range(len(outs))],
        out_shape=[jax.ShapeDtypeStruct(shape, kind) for shape, kind in outs],
        scratch_shapes=[pltpu.VMEM(s, F32) if isinstance(s, tuple) else s for s in scratch],
        compiler_params=pltpu.CompilerParams(vmem_limit_bytes=16 * 1024 * 1024),
    )(*args)


def exchange(x):
    return lax.all_to_all(x, AXES, 0, 0)


def solution(mesh):
    def local(pair, cotangent, token_mask, w_in1, w_out1, w_in2, w_out2):
        rt, ct, c = pair.shape
        h = w_out1.shape[0]
        plan = Plan(mesh, (rt, ct), c, h)
        n, cpd, pos, tokens = plan.n, plan.cpd, plan.pos, plan.tokens
        idx = jnp.stack([lax.axis_index("row"), lax.axis_index("col")]).astype(jnp.int32)
        lanes = (c, pos)
        both = (n, 2 * cpd, pos)
        single = (n, cpd, pos)
        group = plan.lane_groups
        scr1 = (group, tokens * cpd, LANES)
        scr2 = (group, tokens * 2 * cpd, LANES)

        flat = (pos, c)
        dma = pltpu.SemaphoreType.DMA
        halves = (c // 2, 8 * h)
        swap = [(i, i ^ 1) for i in range(plan.cols)]

        lifts = (c, h)
        wide = (2 * h, pos)
        back = (c, 2 * h)
        chip = (plan.wide // LANES, 2 * c, LANES)

        x1, z, mask = call(
            first_kernel(plan), "first", [(both, BF16), (lanes, BF16), ((8, pos), F32)],
            [idx, pair.reshape(flat), token_mask.reshape(1, tokens), w_in1],
            [pltpu.VMEM(flat, BF16), pltpu.VMEM((1, tokens), jnp.int32), pltpu.VMEM((c, 5 * h), BF16), flat, dma((3,))],
            scalars=1, far_in=3,
        )
        y1 = exchange(x1)
        x2, lr1 = call(
            product_kernel(plan, True), "product_out", [(single, BF16), ((2 * cpd, tokens, tokens), BF16)],
            [y1], [scr2, scr1],
        )
        y2 = exchange(x2)
        x3, mid = call(
            middle_kernel(plan), "middle", [(both, BF16), (lanes, BF16)],
            [z, y2, mask, w_in1, w_out1, w_in2], [(h, pos)],
        )
        y3 = exchange(x3)
        x4, lr2 = call(
            product_kernel(plan, False), "product_in", [(single, BF16), ((2 * cpd, tokens, tokens), BF16)],
            [y3], [scr2, scr1],
        )
        y4 = exchange(x4)
        x5, cot = call(
            turn_kernel(plan), "turn", [(single, BF16), (lanes, BF16)],
            [y4, mid, cotangent.reshape(flat), w_in2, w_out2], [(h, pos), flat],
        )
        y5 = exchange(x5)
        (x6,) = call(grad_kernel(plan, False), "grads_in", [(both, BF16)], [y5, lr2], [scr1, scr2])
        y6 = exchange(x6)
        vc2, gc2, vw2, gw2 = call(
            before_back_kernel(plan), "before_back2", [(wide, BF16), (wide, BF16), (back, BF16), (back, BF16)],
            [y5, mid, mask, w_in2], after=1,
        )
        (gate1,) = call(gate_kernel(plan), "gate", [(lanes, F32)], [y5, z, w_in1], after=1)
        updated, dog2, og2, gg2 = call(
            after_turn_kernel(plan), "after_turn", [(flat, BF16), (lanes, BF16), ((h, c), F32), (lifts, F32)],
            [y5, y4, mid, cot, w_in2, w_out2],
            [(h, pos), flat, pltpu.VMEM(flat, BF16), dma(())], after=1, far_out=(0,),
        )
        x7, mid_grad = call(
            back_kernel(plan), "back", [(single, BF16), (lanes, BF16)],
            [y6, vc2, gc2, vw2, gw2, dog2, mid, cot, gate1, w_in2, w_out1, y2], [(h, pos), wide],
        )
        y7 = exchange(x7)
        keep, send, dog1 = call(
            after_back_kernel(plan), "after_back", [(halves, F32), (halves, BF16), (lanes, BF16)],
            [idx, y6, vc2, gc2, mid, mid_grad, gate1, y2, z, og2, gg2, w_out1],
            [(h, pos), wide, (c, 8 * h)], scalars=1,
        )
        other = lax.ppermute(send, "col", swap)
        vc1, gc1, vw1, gw1 = call(
            before_back_kernel(plan), "before_back1", [(wide, BF16), (wide, BF16), (back, BF16), (back, BF16)],
            [dog1, z, mask, w_in1], after=1,
        )
        (x8,) = call(
            grad_kernel(plan, True), "grads_out", [((n, 2 * cpd, pos + plan.wide), BF16)],
            [vw1, y7, lr1, keep, other], [scr1, scr2, chip], after=1,
        )
        y8 = exchange(x8)
        (x9,) = call(
            last_kernel(plan), "last", [((n, cpd, 4 * h + 2 * plan.wide), BF16)], [y8, z, vc1, gc1], [wide]
        )
        y9 = exchange(x9)
        (x10,) = call(sum_kernel(plan), "sum", [((n, cpd, 4 * h), BF16)], [y9])
        y10 = exchange(x10)
        (own,) = call(half_kernel(plan), "half", [((n, cpd, 2 * plan.wide), BF16)], [y9])
        partner = lax.ppermute(own, "col", swap)
        (pair_grad,) = call(
            after_last_kernel(plan), "after_last", [(flat, BF16)],
            [y9, y8, z, mid_grad, dog1, vc1, gc1, vw1, gw1, w_in1],
            [wide, flat, pltpu.VMEM(flat, BF16), dma(())], after=1, far_out=(0,),
        )
        g1, out1, in2, out2 = call(
            assemble_kernel(plan), "assemble",
            [((c, h), F32), ((h, c), F32), ((c, 5 * h), F32), ((h, c), F32)],
            [idx, own, partner], [chip], scalars=1,
        )
        (in1,) = call(end_kernel(plan), "end", [((c, 5 * h), F32)], [y10, g1])
        return updated.reshape(rt, ct, c), pair_grad.reshape(rt, ct, c), in1, out1, in2, out2

    return jax.shard_map(
        local,
        mesh=mesh,
        in_specs=(P("row", "col", None), P("row", "col", None), P(), P(), P(), P(), P()),
        out_specs=(P("row", "col", None), P("row", "col", None), P(), P(), P(), P()),
        check_vma=False,
    )
```

```python
import jax
import jax.numpy as jnp
from jax import lax
from jax.experimental import pallas as pl
from jax.experimental.pallas import tpu as pltpu
from jax.sharding import PartitionSpec as P

EPSILON = 1e-05
LANES = 128
AXES = ("row", "col")
F32 = jnp.float32
BF16 = jnp.bfloat16


class Plan:
    def __init__(self, mesh, tile, width, hidden):
        self.rows = mesh.shape["row"]
        self.cols = mesh.shape["col"]
        self.n = self.rows * self.cols
        self.rt, self.ct = tile
        self.pos = self.rt * self.ct
        self.tokens = self.rt * self.rows
        self.c = width
        self.h = hidden
        self.cpd = hidden // self.n
        self.crow = width // self.n
        self.blocks = LANES // self.rt
        self.lane_groups = self.tokens // LANES
        self.seconds = self.pos // LANES
        self.wide = 8 * hidden // self.n * (width // 2) // (2 * self.crow)
        assert self.blocks >= 1 and self.cpd == self.crow
        assert self.rt & (self.rt - 1) == 0 and self.rows == self.blocks * self.lane_groups


def nn(a, b):
    return jnp.dot(a, b, preferred_element_type=F32)


def nt(a, b):
    return lax.dot_general(a, b, (((1,), (1,)), ((), ())), preferred_element_type=F32)


def iota(shape, axis):
    return lax.broadcasted_iota(jnp.int32, shape, axis)


def one_hot(cond):
    return jnp.where(cond, 1.0, 0.0).astype(BF16)


def eye(size):
    return one_hot(iota((size, size), 0) == iota((size, size), 1))


def to_lanes(tile_ref, scr, plan):
    scr[...] = tile_ref[...].astype(F32)
    rows = [scr[pl.ds(k, plan.rt, stride=plan.ct), :] for k in range(plan.ct)]
    return nt(eye(plan.c), jnp.concatenate(rows, axis=0).astype(BF16))


def from_lanes(lanes, scr, plan):
    turn = eye(LANES)
    for q in range(plan.seconds):
        block = nt(turn, lanes[:, q * LANES : (q + 1) * LANES])
        for b in range(plan.blocks):
            rows = block[b * plan.rt : (b + 1) * plan.rt, :]
            scr[pl.ds(q * plan.blocks + b, plan.rt, stride=plan.ct), :] = rows
    return scr[...].astype(BF16)


def split_order(plan):
    wide = 2 * plan.h
    row = iota((wide, wide), 0)
    source = iota((wide, wide), 1)
    per = 2 * plan.cpd
    bits = per.bit_length() - 1
    side = (row & (per - 1)) >> (bits - 1)
    channel = (row >> bits) * plan.cpd + (row & (plan.cpd - 1))
    return one_hot(source == side * plan.h + channel)


def sides(w, first, plan):
    h = plan.h
    return jnp.concatenate([w[:, first * h : (first + 1) * h], w[:, (first + 2) * h : (first + 3) * h]], axis=1)


def standard(x):
    centre = jnp.mean(x, axis=0, keepdims=True)
    shifted = x - centre
    spread = jnp.mean(shifted * shifted, axis=0, keepdims=True)
    scale = lax.rsqrt(spread + EPSILON)
    return shifted * scale, scale


def standard_grad(unit, scale, grad):
    flat = jnp.mean(grad, axis=0, keepdims=True)
    along = jnp.mean(grad * unit, axis=0, keepdims=True)
    return scale * (grad - flat - unit * along)


def split_weights(w, plan):
    perm = split_order(plan)
    return nt(perm, sides(w, 0, plan)).astype(BF16), nt(perm, sides(w, 1, plan)).astype(BF16)


def split_projection(normed, value_w, gate_w):
    return nn(value_w, normed), jax.nn.sigmoid(nn(gate_w, normed))


def out_gate(normed, w, plan):
    tail = nt(eye(plan.h), w[:, 4 * plan.h :]).astype(BF16)
    return jax.nn.sigmoid(nn(tail, normed))


def back_coefficients(normed, w, mask, plan):
    value, gate = split_projection(normed, *split_weights(w, plan))
    through = gate * mask
    return through, through * value * (1.0 - gate)


def back_weights(w, plan):
    perm = split_order(plan)
    return nt(sides(w, 0, plan), perm).astype(BF16), nt(sides(w, 1, plan), perm).astype(BF16)


def side_terms(normed, value_grad, gate_grad, plan):
    perm = split_order(plan)
    value_part = nn(nt(normed, value_grad).astype(BF16), perm)
    gate_part = nn(nt(normed, gate_grad).astype(BF16), perm)
    h = plan.h
    return [value_part[:, :h], gate_part[:, :h], value_part[:, h:], gate_part[:, h:]]


def put_rows(dest_ref, value, per, plan, start=0):
    size = value.shape[1]
    for d in range(plan.n):
        dest_ref[d, :, start : start + size] = value[per * d : per * (d + 1), :].astype(dest_ref.dtype)


def get_rows(source_ref, scratch_ref, per, plan, start, size):
    for d in range(plan.n):
        scratch_ref[per * d : per * (d + 1), :size] = source_ref[d, :, start : start + size].astype(F32)
    return scratch_ref[:, :size]


def first_kernel(plan):
    def body(idx, pair_hbm, tokens_hbm, w_hbm, x_ref, z_ref, mask_ref, pair, tokens, w_in, scr, sems):
        sources = (pair_hbm, tokens_hbm, w_hbm)
        copies = [
            pltpu.make_async_copy(source, dest, sems.at[i])
            for i, (source, dest) in enumerate(zip(sources, (pair, tokens, w_in)))
        ]
        for copy in copies:
            copy.start()
        token = iota((plan.tokens, plan.pos), 0)
        lane = iota((plan.tokens, plan.pos), 1)
        shift = plan.rt.bit_length() - 1
        first = one_hot(token == idx[0] * plan.rt + (lane & (plan.rt - 1)))
        second = one_hot(token == idx[1] * plan.ct + (lane >> shift))
        copies[1].wait()
        flags = jnp.broadcast_to(tokens[...].astype(F32), (8, plan.tokens)).astype(BF16)
        mask = nn(flags, first) * nn(flags, second)
        mask_ref[...] = mask
        copies[2].wait()
        value_w, gate_w = split_weights(w_in[...], plan)
        copies[0].wait()
        z = to_lanes(pair, scr, plan)
        z_ref[...] = z.astype(BF16)
        value, gate = split_projection(standard(z)[0].astype(BF16), value_w, gate_w)
        put_rows(x_ref, gate * value * mask[:1], 2 * plan.cpd, plan)

    return body


def middle_kernel(plan):
    def body(z_ref, y_ref, mask_ref, w_in1, w_out1, w_in2, x_ref, mid_ref, gate_out, vc_ref, gc_ref, vw_ref, gw_ref, scr):
        z = z_ref[...].astype(F32)
        gate = out_gate(standard(z)[0].astype(BF16), w_in1[...], plan)
        gate_out[...] = gate
        tri = get_rows(y_ref, scr, plan.cpd, plan, 0, plan.pos)
        lifted = nn(nt(eye(plan.c), w_out1[...]).astype(BF16), standard(tri)[0].astype(BF16))
        mid = (z + gate * lifted).astype(BF16)
        mid_ref[...] = mid
        normed = standard(mid.astype(F32))[0].astype(BF16)
        value, gate = split_projection(normed, *split_weights(w_in2[...], plan))
        through = gate * mask_ref[:1, :]
        part = through * value
        put_rows(x_ref, part, 2 * plan.cpd, plan)
        vc_ref[...] = through.astype(BF16)
        gc_ref[...] = (part * (1.0 - gate)).astype(BF16)
        vw_ref[...], gw_ref[...] = back_weights(w_in2[...], plan)

    return body


def turn_kernel(plan):
    def body(y_ref, mid_ref, cot_ref, w_in2, w_out2, x_ref, cot_out, dog_ref, scr, flat):
        cot = to_lanes(cot_ref, flat, plan)
        cot_out[...] = cot.astype(BF16)
        gate = out_gate(standard(mid_ref[...].astype(F32))[0].astype(BF16), w_in2[...], plan)
        lift_grad = (gate * cot).astype(BF16)
        unit, scale = standard(get_rows(y_ref, scr, plan.cpd, plan, 0, plan.pos))
        put_rows(x_ref, standard_grad(unit, scale, nn(w_out2[...], lift_grad)), plan.cpd, plan)
        lifted = nn(nt(eye(plan.c), w_out2[...]).astype(BF16), unit.astype(BF16))
        dog_ref[...] = (lifted * cot * gate * (1.0 - gate)).astype(BF16)

    return body


def after_turn_kernel(plan):
    def body(after, y_ref, mid_ref, cot_ref, dog_ref, w_in2, w_out2, up_hbm, og_ref, gg_ref, scr, flat, up, sem):
        tri = get_rows(y_ref, scr, plan.cpd, plan, 0, plan.pos)
        rounded = standard(tri)[0].astype(BF16)
        lifted = nn(nt(eye(plan.c), w_out2[...]).astype(BF16), rounded)
        mid, cot = mid_ref[...].astype(F32), cot_ref[...].astype(F32)
        normed = standard(mid)[0].astype(BF16)
        gate = out_gate(normed, w_in2[...], plan)
        up[...] = from_lanes((mid + gate * lifted).astype(BF16), flat, plan)
        copy = pltpu.make_async_copy(up, up_hbm, sem)
        copy.start()
        og_ref[...] = nt(rounded, (gate * cot).astype(BF16))
        gg_ref[...] = nt(normed, dog_ref[...])
        copy.wait()

    return body


def before_back_kernel(plan):
    def body(after, source_ref, mask_ref, w_in, vc_ref, gc_ref, vw_ref, gw_ref):
        normed = standard(source_ref[...].astype(F32))[0].astype(BF16)
        value, gate = back_coefficients(normed, w_in[...], mask_ref[:1, :], plan)
        vc_ref[...] = value.astype(BF16)
        gc_ref[...] = gate.astype(BF16)
        vw_ref[...], gw_ref[...] = back_weights(w_in[...], plan)

    return body


def side_grads(y_ref, vc_ref, gc_ref, scr, plan):
    grad = get_rows(y_ref, scr, 2 * plan.cpd, plan, 0, plan.pos)
    return (grad * vc_ref[...].astype(F32)).astype(BF16), (grad * gc_ref[...].astype(F32)).astype(BF16)


def back_kernel(plan):
    def body(y6, vc_ref, gc_ref, vw_ref, gw_ref, dog_ref, mid_ref, cot_ref, gate_ref, w_in2, w_out1, y2,
             x_ref, mg_ref, scr, scr2):
        value_grad, gate_grad = side_grads(y6, vc_ref, gc_ref, scr2, plan)
        normed_grad = nn(vw_ref[...], value_grad) + nn(gw_ref[...], gate_grad)
        normed_grad += nn(w_in2[:, 4 * plan.h :], dog_ref[...])
        unit, scale = standard(mid_ref[...].astype(F32))
        mid_grad = (cot_ref[...].astype(F32) + standard_grad(unit, scale, normed_grad)).astype(BF16)
        mg_ref[...] = mid_grad
        lift_grad = (gate_ref[...] * mid_grad.astype(F32)).astype(BF16)
        unit, scale = standard(get_rows(y2, scr, plan.cpd, plan, 0, plan.pos))
        put_rows(x_ref, standard_grad(unit, scale, nn(w_out1[...], lift_grad)), plan.cpd, plan)

    return body


def after_back_kernel(plan):
    def body(idx, y6, vc_ref, gc_ref, mid_ref, mg_ref, gate_ref, y2, z_ref, og2, gg2, w_out1,
             keep_ref, send_ref, dog_ref, scr, scr2, sums):
        value_grad, gate_grad = side_grads(y6, vc_ref, gc_ref, scr2, plan)
        terms = side_terms(standard(mid_ref[...].astype(F32))[0].astype(BF16), value_grad, gate_grad, plan)
        mid_grad, gate = mg_ref[...].astype(F32), gate_ref[...]
        lift_grad = (gate * mid_grad).astype(BF16)
        rounded = standard(get_rows(y2, scr, plan.cpd, plan, 0, plan.pos))[0].astype(BF16)
        lifted = nn(nt(eye(plan.c), w_out1[...]).astype(BF16), rounded)
        dog = (lifted * mid_grad * gate * (1.0 - gate)).astype(BF16)
        dog_ref[...] = dog
        normed = standard(z_ref[...].astype(F32))[0].astype(BF16)
        terms += [gg2[...], og2[...], nt(rounded, lift_grad), nt(normed, dog)]
        at = 0
        for part in terms:
            sums[:, at : at + part.shape[1]] = part
            at += part.shape[1]
        half = plan.c // 2
        core = idx[1] & 1
        keep_ref[...] = sums[pl.ds(pl.multiple_of(core * half, 8), half), :]
        send_ref[...] = sums[pl.ds(pl.multiple_of((1 - core) * half, 8), half), :].astype(BF16)

    return body


def last_kernel(plan):
    def body(y8, z_ref, vc_ref, gc_ref, x_ref, scr):
        crow, wide = plan.crow, plan.wide
        value_grad, gate_grad = side_grads(y8, vc_ref, gc_ref, scr, plan)
        normed = standard(z_ref[...].astype(F32))[0].astype(BF16)
        at = 0
        for part in side_terms(normed, value_grad, gate_grad, plan):
            put_rows(x_ref, part, crow, plan, at)
            at += part.shape[1]
        for core in range(2):
            total = y8[core, :, plan.pos :].astype(F32)
            for d in range(core + 2, plan.n, 2):
                total = total + y8[d, :, plan.pos :].astype(F32)
            total = (total * (1.0 / plan.tokens)).astype(BF16)
            for d in range(core, plan.n, 2):
                x_ref[d, :, at : at + wide] = total[:crow, :]
                x_ref[d, :, at + wide :] = total[crow:, :]

    return body


def after_last_kernel(plan):
    def body(after, y8, z_ref, mg_ref, dog_ref, vc_ref, gc_ref, vw_ref, gw_ref, w_in1, pg_hbm, scr, flat, pg, sem):
        value_grad, gate_grad = side_grads(y8, vc_ref, gc_ref, scr, plan)
        normed_grad = nn(vw_ref[...], value_grad) + nn(gw_ref[...], gate_grad)
        normed_grad += nn(w_in1[:, 4 * plan.h :], dog_ref[...])
        unit, scale = standard(z_ref[...].astype(F32))
        grad = mg_ref[...].astype(F32) + standard_grad(unit, scale, normed_grad)
        pg[...] = from_lanes(grad.astype(BF16), flat, plan)
        copy = pltpu.make_async_copy(pg, pg_hbm, sem)
        copy.start()
        copy.wait()

    return body


def sum_kernel(plan):
    def body(y_ref, x_ref):
        width = 4 * plan.h
        total = y_ref[0, :, :width].astype(F32)
        for d in range(1, plan.n):
            total = total + y_ref[d, :, :width].astype(F32)
        total = (total * (1.0 / plan.tokens)).astype(BF16)
        for d in range(plan.n):
            x_ref[d] = total

    return body


def half_kernel(plan):
    def body(y_ref, half_ref):
        half_ref[...] = y_ref[:, :, 4 * plan.h :]

    return body


def assemble_kernel(plan):
    def body(idx, own_ref, other_ref, g1_ref, out1_ref, in2_ref, out2_ref, scr):
        h, crow, wide = plan.h, plan.crow, plan.wide
        half = plan.c // 2
        steps = 8 * h // wide
        per = 2 * crow
        outs = ((in2_ref, 5 * h), (out2_ref, h), (out1_ref, h), (g1_ref, h))
        for k, ref in enumerate((own_ref, other_ref)):
            for d in range(plan.n):
                for g in range(wide // LANES):
                    scr[g, per * d : per * d + crow, :] = ref[d, :, g * LANES : (g + 1) * LANES].astype(F32)
                    scr[g, per * d + crow : per * (d + 1), :] = ref[
                        d, :, wide + g * LANES : wide + (g + 1) * LANES
                    ].astype(F32)
            core = idx[1] & 1 if k == 0 else 1 - (idx[1] & 1)
            rows = pl.ds(pl.multiple_of(core * half, 8), half)
            pieces = [
                scr[g, pl.ds(v, half, stride=steps), :] for v in range(steps) for g in range(wide // LANES)
            ]
            for out_ref, size in outs:
                for i in range(size // LANES):
                    out_ref[rows, i * LANES : (i + 1) * LANES] = pieces.pop(0)

    return body


def end_kernel(plan):
    def body(y_ref, g1_ref, in1_ref):
        crow, width = plan.crow, 4 * plan.h
        for d in range(plan.n):
            in1_ref[crow * d : crow * (d + 1), :width] = y_ref[d].astype(F32)
        in1_ref[:, width:] = g1_ref[...]

    return body


def turn_blocks(group, plan):
    count, size = plan.blocks, plan.rt
    lane = iota(group[0].shape, 1)
    group = list(group)
    step = count // 2
    while step:
        low = (lane & (step * size)) == 0
        for a in range(count):
            if a & step == 0:
                x, y = group[a], group[a + step]
                group[a] = jnp.where(low, x, pltpu.roll(y, step * size, 1))
                group[a + step] = jnp.where(low, pltpu.roll(x, LANES - step * size, 1), y)
        step //= 2
    return group


def spread(y_ref, scr, per, plan):
    for c in range(plan.cols):
        for g in range(plan.lane_groups):
            for q in range(plan.seconds):
                group = []
                for b in range(plan.blocks):
                    src = (g * plan.blocks + b) * plan.cols + c
                    group.append(y_ref[src, :per, q * LANES : (q + 1) * LANES].astype(F32))
                group = turn_blocks(group, plan)
                for b in range(plan.blocks):
                    second = c * plan.ct + q * plan.blocks + b
                    scr[g, second * per : (second + 1) * per, :] = group[b]


def collect(scr, x_ref, per, plan):
    for c in range(plan.cols):
        for g in range(plan.lane_groups):
            for q in range(plan.seconds):
                group = []
                for b in range(plan.blocks):
                    second = c * plan.ct + q * plan.blocks + b
                    group.append(scr[g, second * per : (second + 1) * per, :])
                group = turn_blocks(group, plan)
                for b in range(plan.blocks):
                    dest = (g * plan.blocks + b) * plan.cols + c
                    x_ref[dest, :per, q * LANES : (q + 1) * LANES] = group[b].astype(BF16)


def pick(scr, row, per, plan):
    parts = [scr[g, pl.ds(row, plan.tokens, stride=per), :] for g in range(plan.lane_groups)]
    return parts[0] if len(parts) == 1 else jnp.concatenate(parts, axis=1)


def place(scr, row, per, value, plan):
    for g in range(plan.lane_groups):
        scr[g, pl.ds(row, plan.tokens, stride=per), :] = value[:, g * LANES : (g + 1) * LANES]


def product_kernel(plan, outgoing):
    cpd = plan.cpd

    def body(y_ref, x_ref, lr_ref, scr, scr_out):
        turn = eye(plan.tokens)
        spread(y_ref, scr, 2 * cpd, plan)
        for t in range(cpd):
            left_b = pick(scr, t, 2 * cpd, plan).astype(BF16)
            right_b = pick(scr, cpd + t, 2 * cpd, plan).astype(BF16)
            lr_ref[t] = left_b
            lr_ref[cpd + t] = right_b
            tri = nn(nt(turn, right_b).astype(BF16), left_b) if outgoing else nt(right_b, left_b)
            place(scr_out, t, cpd, tri, plan)
        collect(scr_out, x_ref, cpd, plan)

    return body


def grad_kernel(plan, outgoing):
    cpd = plan.cpd

    def body(*refs):
        if outgoing:
            after, y_ref, lr_ref, keep_ref, other_ref, x_ref, scr, scr_out, scr_sum = refs
        else:
            y_ref, lr_ref, x_ref, scr, scr_out = refs
        turn = eye(plan.tokens)
        spread(y_ref, scr, cpd, plan)
        for t in range(cpd):
            grad_b = pick(scr, t, cpd, plan).astype(BF16)
            left, right = lr_ref[t], lr_ref[cpd + t]
            if outgoing:
                left_grad, right_grad = nn(right, grad_b), nt(left, grad_b)
            else:
                left_grad, right_grad = nn(nt(turn, grad_b).astype(BF16), right), nn(grad_b, left)
            place(scr_out, t, 2 * cpd, left_grad, plan)
            place(scr_out, cpd + t, 2 * cpd, right_grad, plan)
        collect(scr_out, x_ref, 2 * cpd, plan)
        if outgoing:
            half, wide, per = plan.c // 2, plan.wide, 2 * plan.crow
            steps = 8 * plan.h // wide
            total = keep_ref[...] + other_ref[...].astype(F32)
            for v in range(steps):
                for g in range(wide // LANES):
                    at = v * wide + g * LANES
                    scr_sum[g, pl.ds(v, half, stride=steps), :] = total[:, at : at + LANES]
            for d in range(plan.n):
                for g in range(wide // LANES):
                    at = plan.pos + g * LANES
                    x_ref[d, :, at : at + LANES] = scr_sum[g, per * d : per * (d + 1), :].astype(BF16)

    return body


def call(body, name, outs, args, scratch=(), scalars=0, far_in=0, after=0, far_out=()):
    near = pl.BlockSpec(memory_space=pltpu.VMEM)
    far = pl.BlockSpec(memory_space=pltpu.HBM)
    ins = [pl.BlockSpec(memory_space=pltpu.SMEM)] * scalars + [far] * far_in
    args = [
        pltpu.with_memory_space_constraint(a, pltpu.HBM) if scalars <= i < len(ins) else a for i, a in enumerate(args)
    ]
    ins += [pl.BlockSpec(memory_space=pl.ANY)] * after
    return pl.pallas_call(
        body,
        name=name,
        in_specs=ins + [near] * (len(args) - len(ins)),
        out_specs=[far if i in far_out else near for i in range(len(outs))],
        out_shape=[jax.ShapeDtypeStruct(shape, kind) for shape, kind in outs],
        scratch_shapes=[pltpu.VMEM(s, F32) if isinstance(s, tuple) else s for s in scratch],
        compiler_params=pltpu.CompilerParams(vmem_limit_bytes=16 * 1024 * 1024),
    )(*args)


def exchange(x):
    return lax.all_to_all(x, AXES, 0, 0)


def solution(mesh):
    def local(pair, cotangent, token_mask, w_in1, w_out1, w_in2, w_out2):
        rt, ct, c = pair.shape
        h = w_out1.shape[0]
        plan = Plan(mesh, (rt, ct), c, h)
        n, cpd, pos, tokens = plan.n, plan.cpd, plan.pos, plan.tokens
        idx = jnp.stack([lax.axis_index("row"), lax.axis_index("col")]).astype(jnp.int32)
        lanes = (c, pos)
        both = (n, 2 * cpd, pos)
        single = (n, cpd, pos)
        group = plan.lane_groups
        scr1 = (group, tokens * cpd, LANES)
        scr2 = (group, tokens * 2 * cpd, LANES)

        flat = (pos, c)
        dma = pltpu.SemaphoreType.DMA
        halves = (c // 2, 8 * h)
        swap = [(i, i ^ 1) for i in range(plan.cols)]

        lifts = (c, h)
        wide = (2 * h, pos)
        back = (c, 2 * h)
        chip = (plan.wide // LANES, 2 * c, LANES)

        x1, z, mask = call(
            first_kernel(plan), "first", [(both, BF16), (lanes, BF16), ((8, pos), F32)],
            [idx, pair.reshape(flat), token_mask.reshape(1, tokens), w_in1],
            [pltpu.VMEM(flat, BF16), pltpu.VMEM((1, tokens), jnp.int32), pltpu.VMEM((c, 5 * h), BF16), flat, dma((3,))],
            scalars=1, far_in=3,
        )
        y1 = exchange(x1)
        x2, lr1 = call(
            product_kernel(plan, True), "product_out", [(single, BF16), ((2 * cpd, tokens, tokens), BF16)],
            [y1], [scr2, scr1],
        )
        y2 = exchange(x2)
        x3, mid, gate1, vc2, gc2, vw2, gw2 = call(
            middle_kernel(plan), "middle",
            [(both, BF16), (lanes, BF16), (lanes, F32), (wide, BF16), (wide, BF16), (back, BF16), (back, BF16)],
            [z, y2, mask, w_in1, w_out1, w_in2], [(h, pos)],
        )
        y3 = exchange(x3)
        x4, lr2 = call(
            product_kernel(plan, False), "product_in", [(single, BF16), ((2 * cpd, tokens, tokens), BF16)],
            [y3], [scr2, scr1],
        )
        y4 = exchange(x4)
        x5, cot, dog2 = call(
            turn_kernel(plan), "turn", [(single, BF16), (lanes, BF16), (lanes, BF16)],
            [y4, mid, cotangent.reshape(flat), w_in2, w_out2], [(h, pos), flat],
        )
        y5 = exchange(x5)
        (x6,) = call(grad_kernel(plan, False), "grads_in", [(both, BF16)], [y5, lr2], [scr1, scr2])
        y6 = exchange(x6)
        x7, mid_grad = call(
            back_kernel(plan), "back", [(single, BF16), (lanes, BF16)],
            [y6, vc2, gc2, vw2, gw2, dog2, mid, cot, gate1, w_in2, w_out1, y2], [(h, pos), wide],
        )
        y7 = exchange(x7)
        updated, og2, gg2 = call(
            after_turn_kernel(plan), "after_turn", [(flat, BF16), ((h, c), F32), (lifts, F32)],
            [mid_grad, y4, mid, cot, dog2, w_in2, w_out2],
            [(h, pos), flat, pltpu.VMEM(flat, BF16), dma(())], after=1, far_out=(0,),
        )
        keep, send, dog1 = call(
            after_back_kernel(plan), "after_back", [(halves, F32), (halves, BF16), (lanes, BF16)],
            [idx, y6, vc2, gc2, mid, mid_grad, gate1, y2, z, og2, gg2, w_out1],
            [(h, pos), wide, (c, 8 * h)], scalars=1,
        )
        other = lax.ppermute(send, "col", swap)
        vc1, gc1, vw1, gw1 = call(
            before_back_kernel(plan), "before_back1", [(wide, BF16), (wide, BF16), (back, BF16), (back, BF16)],
            [dog1, z, mask, w_in1], after=1,
        )
        (x8,) = call(
            grad_kernel(plan, True), "grads_out", [((n, 2 * cpd, pos + plan.wide), BF16)],
            [vw1, y7, lr1, keep, other], [scr1, scr2, chip], after=1,
        )
        y8 = exchange(x8)
        (x9,) = call(
            last_kernel(plan), "last", [((n, cpd, 4 * h + 2 * plan.wide), BF16)], [y8, z, vc1, gc1], [wide]
        )
        y9 = exchange(x9)
        (x10,) = call(sum_kernel(plan), "sum", [((n, cpd, 4 * h), BF16)], [y9])
        y10 = exchange(x10)
        (own,) = call(half_kernel(plan), "half", [((n, cpd, 2 * plan.wide), BF16)], [y9])
        partner = lax.ppermute(own, "col", swap)
        (pair_grad,) = call(
            after_last_kernel(plan), "after_last", [(flat, BF16)],
            [y9, y8, z, mid_grad, dog1, vc1, gc1, vw1, gw1, w_in1],
            [wide, flat, pltpu.VMEM(flat, BF16), dma(())], after=1, far_out=(0,),
        )
        g1, out1, in2, out2 = call(
            assemble_kernel(plan), "assemble",
            [((c, h), F32), ((h, c), F32), ((c, 5 * h), F32), ((h, c), F32)],
            [idx, own, partner], [chip], scalars=1,
        )
        (in1,) = call(end_kernel(plan), "end", [((c, 5 * h), F32)], [y10, g1])
        return updated.reshape(rt, ct, c), pair_grad.reshape(rt, ct, c), in1, out1, in2, out2

    return jax.shard_map(
        local,
        mesh=mesh,
        in_specs=(P("row", "col", None), P("row", "col", None), P(), P(), P(), P(), P()),
        out_specs=(P("row", "col", None), P("row", "col", None), P(), P(), P(), P()),
        check_vma=False,
    )
```

```python
import jax
import jax.numpy as jnp
from jax import lax
from jax.experimental import pallas as pl
from jax.experimental.pallas import tpu as pltpu
from jax.sharding import PartitionSpec as P

EPSILON = 1e-05
LANES = 128
AXES = ("row", "col")
F32 = jnp.float32
BF16 = jnp.bfloat16


class Plan:
    def __init__(self, mesh, tile, width, hidden):
        self.rows = mesh.shape["row"]
        self.cols = mesh.shape["col"]
        self.n = self.rows * self.cols
        self.rt, self.ct = tile
        self.pos = self.rt * self.ct
        self.tokens = self.rt * self.rows
        self.c = width
        self.h = hidden
        self.cpd = hidden // self.n
        self.crow = width // self.n
        self.blocks = LANES // self.rt
        self.lane_groups = self.tokens // LANES
        self.seconds = self.pos // LANES
        self.wide = 8 * hidden // self.n * (width // 2) // (2 * self.crow)
        assert self.blocks >= 1 and self.cpd == self.crow
        assert self.rt & (self.rt - 1) == 0 and self.rows == self.blocks * self.lane_groups


def nn(a, b):
    return jnp.dot(a, b, preferred_element_type=F32)


def nt(a, b):
    return lax.dot_general(a, b, (((1,), (1,)), ((), ())), preferred_element_type=F32)


def iota(shape, axis):
    return lax.broadcasted_iota(jnp.int32, shape, axis)


def one_hot(cond):
    return jnp.where(cond, 1.0, 0.0).astype(BF16)


def eye(size):
    return one_hot(iota((size, size), 0) == iota((size, size), 1))


def to_lanes(tile_ref, scr, plan):
    scr[...] = tile_ref[...].astype(F32)
    rows = [scr[pl.ds(k, plan.rt, stride=plan.ct), :] for k in range(plan.ct)]
    return nt(eye(plan.c), jnp.concatenate(rows, axis=0).astype(BF16))


def from_lanes(lanes, scr, plan):
    turn = eye(LANES)
    for q in range(plan.seconds):
        block = nt(turn, lanes[:, q * LANES : (q + 1) * LANES])
        for b in range(plan.blocks):
            rows = block[b * plan.rt : (b + 1) * plan.rt, :]
            scr[pl.ds(q * plan.blocks + b, plan.rt, stride=plan.ct), :] = rows
    return scr[...].astype(BF16)


def split_order(plan):
    wide = 2 * plan.h
    row = iota((wide, wide), 0)
    source = iota((wide, wide), 1)
    per = 2 * plan.cpd
    bits = per.bit_length() - 1
    side = (row & (per - 1)) >> (bits - 1)
    channel = (row >> bits) * plan.cpd + (row & (plan.cpd - 1))
    return one_hot(source == side * plan.h + channel)


def sides(w, first, plan):
    h = plan.h
    return jnp.concatenate([w[:, first * h : (first + 1) * h], w[:, (first + 2) * h : (first + 3) * h]], axis=1)


def standard(x):
    centre = jnp.mean(x, axis=0, keepdims=True)
    shifted = x - centre
    spread = jnp.mean(shifted * shifted, axis=0, keepdims=True)
    scale = lax.rsqrt(spread + EPSILON)
    return shifted * scale, scale


def standard_grad(unit, scale, grad):
    flat = jnp.mean(grad, axis=0, keepdims=True)
    along = jnp.mean(grad * unit, axis=0, keepdims=True)
    return scale * (grad - flat - unit * along)


def split_weights(w, plan):
    perm = split_order(plan)
    return nt(perm, sides(w, 0, plan)).astype(BF16), nt(perm, sides(w, 1, plan)).astype(BF16)


def split_projection(normed, value_w, gate_w):
    return nn(value_w, normed), jax.nn.sigmoid(nn(gate_w, normed))


def out_gate(normed, w, plan):
    tail = nt(eye(plan.h), w[:, 4 * plan.h :]).astype(BF16)
    return jax.nn.sigmoid(nn(tail, normed))


def back_coefficients(normed, w, mask, plan):
    value, gate = split_projection(normed, *split_weights(w, plan))
    through = gate * mask
    return through, through * value * (1.0 - gate)


def back_weights(w, plan):
    perm = split_order(plan)
    return nt(sides(w, 0, plan), perm).astype(BF16), nt(sides(w, 1, plan), perm).astype(BF16)


def side_terms(normed, value_grad, gate_grad, plan):
    perm = split_order(plan)
    value_part = nn(nt(normed, value_grad).astype(BF16), perm)
    gate_part = nn(nt(normed, gate_grad).astype(BF16), perm)
    h = plan.h
    return [value_part[:, :h], gate_part[:, :h], value_part[:, h:], gate_part[:, h:]]


def put_rows(dest_ref, value, per, plan, start=0):
    size = value.shape[1]
    for d in range(plan.n):
        dest_ref[d, :, start : start + size] = value[per * d : per * (d + 1), :].astype(dest_ref.dtype)


def get_rows(source_ref, scratch_ref, per, plan, start, size):
    for d in range(plan.n):
        scratch_ref[per * d : per * (d + 1), :size] = source_ref[d, :, start : start + size].astype(F32)
    return scratch_ref[:, :size]


def first_kernel(plan):
    def body(idx, pair_hbm, tokens_hbm, w_hbm, x_ref, z_ref, mask_ref, pair, tokens, w_in, scr, sems):
        sources = (pair_hbm, tokens_hbm, w_hbm)
        copies = [
            pltpu.make_async_copy(source, dest, sems.at[i])
            for i, (source, dest) in enumerate(zip(sources, (pair, tokens, w_in)))
        ]
        for copy in copies:
            copy.start()
        token = iota((plan.tokens, plan.pos), 0)
        lane = iota((plan.tokens, plan.pos), 1)
        shift = plan.rt.bit_length() - 1
        first = one_hot(token == idx[0] * plan.rt + (lane & (plan.rt - 1)))
        second = one_hot(token == idx[1] * plan.ct + (lane >> shift))
        copies[1].wait()
        flags = jnp.broadcast_to(tokens[...].astype(F32), (8, plan.tokens)).astype(BF16)
        mask = nn(flags, first) * nn(flags, second)
        mask_ref[...] = mask
        copies[2].wait()
        value_w, gate_w = split_weights(w_in[...], plan)
        copies[0].wait()
        z = to_lanes(pair, scr, plan)
        z_ref[...] = z.astype(BF16)
        value, gate = split_projection(standard(z)[0].astype(BF16), value_w, gate_w)
        put_rows(x_ref, gate * value * mask[:1], 2 * plan.cpd, plan)

    return body


def middle_kernel(plan):
    def body(z_ref, y_ref, mask_ref, w_in1, w_out1, w_in2, x_ref, mid_ref, gate_out, vc_ref, gc_ref, vw_ref, gw_ref, scr):
        z = z_ref[...].astype(F32)
        gate = out_gate(standard(z)[0].astype(BF16), w_in1[...], plan)
        gate_out[...] = gate
        tri = get_rows(y_ref, scr, plan.cpd, plan, 0, plan.pos)
        lifted = nn(nt(eye(plan.c), w_out1[...]).astype(BF16), standard(tri)[0].astype(BF16))
        mid = (z + gate * lifted).astype(BF16)
        mid_ref[...] = mid
        normed = standard(mid.astype(F32))[0].astype(BF16)
        value, gate = split_projection(normed, *split_weights(w_in2[...], plan))
        through = gate * mask_ref[:1, :]
        part = through * value
        put_rows(x_ref, part, 2 * plan.cpd, plan)
        vc_ref[...] = through.astype(BF16)
        gc_ref[...] = (part * (1.0 - gate)).astype(BF16)
        vw_ref[...], gw_ref[...] = back_weights(w_in2[...], plan)

    return body


def turn_kernel(plan):
    def body(y_ref, mid_ref, cot_ref, w_in2, w_out2, x_ref, cot_out, dog_ref, scr, flat):
        cot = to_lanes(cot_ref, flat, plan)
        cot_out[...] = cot.astype(BF16)
        gate = out_gate(standard(mid_ref[...].astype(F32))[0].astype(BF16), w_in2[...], plan)
        lift_grad = (gate * cot).astype(BF16)
        unit, scale = standard(get_rows(y_ref, scr, plan.cpd, plan, 0, plan.pos))
        put_rows(x_ref, standard_grad(unit, scale, nn(w_out2[...], lift_grad)), plan.cpd, plan)
        lifted = nn(nt(eye(plan.c), w_out2[...]).astype(BF16), unit.astype(BF16))
        dog_ref[...] = (lifted * cot * gate * (1.0 - gate)).astype(BF16)

    return body


def after_turn_kernel(plan):
    def body(after, y_ref, mid_ref, cot_ref, dog_ref, w_in2, w_out2, up_hbm, og_ref, gg_ref, scr, flat, up, sem):
        tri = get_rows(y_ref, scr, plan.cpd, plan, 0, plan.pos)
        rounded = standard(tri)[0].astype(BF16)
        lifted = nn(nt(eye(plan.c), w_out2[...]).astype(BF16), rounded)
        mid, cot = mid_ref[...].astype(F32), cot_ref[...].astype(F32)
        normed = standard(mid)[0].astype(BF16)
        gate = out_gate(normed, w_in2[...], plan)
        up[...] = from_lanes((mid + gate * lifted).astype(BF16), flat, plan)
        copy = pltpu.make_async_copy(up, up_hbm, sem)
        copy.start()
        og_ref[...] = nt(rounded, (gate * cot).astype(BF16))
        gg_ref[...] = nt(normed, dog_ref[...])
        copy.wait()

    return body


def before_back_kernel(plan):
    def body(after, source_ref, mask_ref, w_in, vc_ref, gc_ref, vw_ref, gw_ref):
        normed = standard(source_ref[...].astype(F32))[0].astype(BF16)
        value, gate = back_coefficients(normed, w_in[...], mask_ref[:1, :], plan)
        vc_ref[...] = value.astype(BF16)
        gc_ref[...] = gate.astype(BF16)
        vw_ref[...], gw_ref[...] = back_weights(w_in[...], plan)

    return body


def side_grads(y_ref, vc_ref, gc_ref, scr, plan):
    grad = get_rows(y_ref, scr, 2 * plan.cpd, plan, 0, plan.pos)
    return (grad * vc_ref[...].astype(F32)).astype(BF16), (grad * gc_ref[...].astype(F32)).astype(BF16)


def back_kernel(plan):
    def body(y6, vc_ref, gc_ref, vw_ref, gw_ref, dog_ref, mid_ref, cot_ref, gate_ref, w_in2, w_out1, y2,
             x_ref, mg_ref, scr, scr2):
        value_grad, gate_grad = side_grads(y6, vc_ref, gc_ref, scr2, plan)
        normed_grad = nn(vw_ref[...], value_grad) + nn(gw_ref[...], gate_grad)
        normed_grad += nn(w_in2[:, 4 * plan.h :], dog_ref[...])
        unit, scale = standard(mid_ref[...].astype(F32))
        mid_grad = (cot_ref[...].astype(F32) + standard_grad(unit, scale, normed_grad)).astype(BF16)
        mg_ref[...] = mid_grad
        lift_grad = (gate_ref[...] * mid_grad.astype(F32)).astype(BF16)
        unit, scale = standard(get_rows(y2, scr, plan.cpd, plan, 0, plan.pos))
        put_rows(x_ref, standard_grad(unit, scale, nn(w_out1[...], lift_grad)), plan.cpd, plan)

    return body


def after_back_kernel(plan):
    def body(idx, y6, vc_ref, gc_ref, mid_ref, mg_ref, gate_ref, y2, z_ref, og2, gg2, w_out1,
             keep_ref, send_ref, dog_ref, scr, scr2, sums):
        value_grad, gate_grad = side_grads(y6, vc_ref, gc_ref, scr2, plan)
        terms = side_terms(standard(mid_ref[...].astype(F32))[0].astype(BF16), value_grad, gate_grad, plan)
        mid_grad, gate = mg_ref[...].astype(F32), gate_ref[...]
        lift_grad = (gate * mid_grad).astype(BF16)
        rounded = standard(get_rows(y2, scr, plan.cpd, plan, 0, plan.pos))[0].astype(BF16)
        lifted = nn(nt(eye(plan.c), w_out1[...]).astype(BF16), rounded)
        dog = (lifted * mid_grad * gate * (1.0 - gate)).astype(BF16)
        dog_ref[...] = dog
        normed = standard(z_ref[...].astype(F32))[0].astype(BF16)
        terms += [gg2[...], og2[...], nt(rounded, lift_grad), nt(normed, dog)]
        at = 0
        for part in terms:
            sums[:, at : at + part.shape[1]] = part
            at += part.shape[1]
        half = plan.c // 2
        core = idx[1] & 1
        keep_ref[...] = sums[pl.ds(pl.multiple_of(core * half, 8), half), :]
        send_ref[...] = sums[pl.ds(pl.multiple_of((1 - core) * half, 8), half), :].astype(BF16)

    return body


def last_kernel(plan):
    def body(y8, z_ref, vc_ref, gc_ref, x_ref, scr):
        crow, wide = plan.crow, plan.wide
        value_grad, gate_grad = side_grads(y8, vc_ref, gc_ref, scr, plan)
        normed = standard(z_ref[...].astype(F32))[0].astype(BF16)
        at = 0
        for part in side_terms(normed, value_grad, gate_grad, plan):
            put_rows(x_ref, part, crow, plan, at)
            at += part.shape[1]
        for core in range(2):
            total = y8[core, :, plan.pos :].astype(F32)
            for d in range(core + 2, plan.n, 2):
                total = total + y8[d, :, plan.pos :].astype(F32)
            total = (total * (1.0 / plan.tokens)).astype(BF16)
            for d in range(core, plan.n, 2):
                x_ref[d, :, at : at + wide] = total[:crow, :]
                x_ref[d, :, at + wide :] = total[crow:, :]

    return body


def after_last_kernel(plan):
    def body(after, y8, z_ref, mg_ref, dog_ref, vc_ref, gc_ref, vw_ref, gw_ref, w_in1, pg_hbm, scr, flat, pg, sem):
        value_grad, gate_grad = side_grads(y8, vc_ref, gc_ref, scr, plan)
        normed_grad = nn(vw_ref[...], value_grad) + nn(gw_ref[...], gate_grad)
        normed_grad += nn(w_in1[:, 4 * plan.h :], dog_ref[...])
        unit, scale = standard(z_ref[...].astype(F32))
        grad = mg_ref[...].astype(F32) + standard_grad(unit, scale, normed_grad)
        pg[...] = from_lanes(grad.astype(BF16), flat, plan)
        copy = pltpu.make_async_copy(pg, pg_hbm, sem)
        copy.start()
        copy.wait()

    return body


def sum_kernel(plan):
    def body(y_ref, x_ref):
        width = 4 * plan.h
        total = y_ref[0, :, :width].astype(F32)
        for d in range(1, plan.n):
            total = total + y_ref[d, :, :width].astype(F32)
        total = (total * (1.0 / plan.tokens)).astype(BF16)
        for d in range(plan.n):
            x_ref[d] = total

    return body


def half_kernel(plan):
    def body(y_ref, half_ref):
        half_ref[...] = y_ref[:, :, 4 * plan.h :]

    return body


def assemble_kernel(plan):
    def body(idx, own_ref, other_ref, g1_ref, out1_ref, in2_ref, out2_ref, scr):
        h, crow, wide = plan.h, plan.crow, plan.wide
        half = plan.c // 2
        steps = 8 * h // wide
        per = 2 * crow
        outs = ((in2_ref, 5 * h), (out2_ref, h), (out1_ref, h), (g1_ref, h))
        for k, ref in enumerate((own_ref, other_ref)):
            for d in range(plan.n):
                for g in range(wide // LANES):
                    scr[g, per * d : per * d + crow, :] = ref[d, :, g * LANES : (g + 1) * LANES].astype(F32)
                    scr[g, per * d + crow : per * (d + 1), :] = ref[
                        d, :, wide + g * LANES : wide + (g + 1) * LANES
                    ].astype(F32)
            core = idx[1] & 1 if k == 0 else 1 - (idx[1] & 1)
            rows = pl.ds(pl.multiple_of(core * half, 8), half)
            pieces = [
                scr[g, pl.ds(v, half, stride=steps), :] for v in range(steps) for g in range(wide // LANES)
            ]
            for out_ref, size in outs:
                for i in range(size // LANES):
                    out_ref[rows, i * LANES : (i + 1) * LANES] = pieces.pop(0)

    return body


def end_kernel(plan):
    def body(y_ref, g1_ref, in1_ref):
        crow, width = plan.crow, 4 * plan.h
        for d in range(plan.n):
            in1_ref[crow * d : crow * (d + 1), :width] = y_ref[d].astype(F32)
        in1_ref[:, width:] = g1_ref[...]

    return body


def turn_blocks(group, plan):
    count, size = plan.blocks, plan.rt
    lane = iota(group[0].shape, 1)
    group = list(group)
    step = count // 2
    while step:
        low = (lane & (step * size)) == 0
        for a in range(count):
            if a & step == 0:
                x, y = group[a], group[a + step]
                group[a] = jnp.where(low, x, pltpu.roll(y, step * size, 1))
                group[a + step] = jnp.where(low, pltpu.roll(x, LANES - step * size, 1), y)
        step //= 2
    return group


def spread(y_ref, scr, per, plan, steps=1):
    def column(c, carry):
        for g in range(plan.lane_groups):
            for q in range(plan.seconds):
                group = []
                for b in range(plan.blocks):
                    src = (g * plan.blocks + b) * plan.cols + c
                    group.append(y_ref[src, :per, q * LANES : (q + 1) * LANES].astype(F32))
                group = turn_blocks(group, plan)
                for b in range(plan.blocks):
                    row = pl.multiple_of((c * plan.ct + q * plan.blocks + b) * per, per)
                    scr[g, pl.ds(row, per), :] = group[b]
        return carry

    lax.fori_loop(0, plan.cols, column, 0, unroll=plan.cols // steps)


def collect(scr, x_ref, per, plan):
    def column(c, carry):
        for g in range(plan.lane_groups):
            for q in range(plan.seconds):
                group = []
                for b in range(plan.blocks):
                    row = pl.multiple_of((c * plan.ct + q * plan.blocks + b) * per, per)
                    group.append(scr[g, pl.ds(row, per), :])
                group = turn_blocks(group, plan)
                for b in range(plan.blocks):
                    dest = (g * plan.blocks + b) * plan.cols + c
                    x_ref[dest, :per, q * LANES : (q + 1) * LANES] = group[b].astype(BF16)
        return carry

    lax.fori_loop(0, plan.cols, column, 0, unroll=plan.cols)


def pick(scr, row, per, plan):
    parts = [scr[g, pl.ds(row, plan.tokens, stride=per), :] for g in range(plan.lane_groups)]
    return parts[0] if len(parts) == 1 else jnp.concatenate(parts, axis=1)


def place(scr, row, per, value, plan):
    for g in range(plan.lane_groups):
        scr[g, pl.ds(row, plan.tokens, stride=per), :] = value[:, g * LANES : (g + 1) * LANES]


def product_kernel(plan, outgoing):
    cpd = plan.cpd

    def body(y_ref, x_ref, lr_ref, scr, scr_out):
        turn = eye(plan.tokens)
        spread(y_ref, scr, 2 * cpd, plan, 1 if outgoing else 2)
        sides = [pick(scr, row, 2 * cpd, plan).astype(BF16) for row in range(2 * cpd)]
        for row, side in enumerate(sides):
            lr_ref[row] = side
        left, right = sides[:cpd], sides[cpd:]
        if outgoing:
            right = [nt(turn, side).astype(BF16) for side in right]
        for t, tri in enumerate([nn(b, a) if outgoing else nt(b, a) for a, b in zip(left, right)]):
            place(scr_out, t, cpd, tri, plan)
        collect(scr_out, x_ref, cpd, plan)

    return body


def grad_kernel(plan, outgoing):
    cpd = plan.cpd

    def body(*refs):
        if outgoing:
            after, y_ref, lr_ref, keep_ref, other_ref, x_ref, scr, scr_out, scr_sum = refs
        else:
            y_ref, lr_ref, x_ref, scr, scr_out = refs
        turn = eye(plan.tokens)
        spread(y_ref, scr, cpd, plan, 2 if outgoing else 1)
        left = [lr_ref[t] for t in range(cpd)]
        right = [lr_ref[cpd + t] for t in range(cpd)]
        grads = [pick(scr, t, cpd, plan).astype(BF16) for t in range(cpd)]
        if outgoing:
            terms = [nn(b, grad) for b, grad in zip(right, grads)] + [nt(a, grad) for a, grad in zip(left, grads)]
        else:
            turned = [nt(turn, grad).astype(BF16) for grad in grads]
            terms = [nn(grad, b) for b, grad in zip(right, turned)] + [nn(grad, a) for a, grad in zip(left, grads)]
        for row, term in enumerate(terms):
            place(scr_out, row, 2 * cpd, term, plan)
        collect(scr_out, x_ref, 2 * cpd, plan)
        if outgoing:
            half, wide, per = plan.c // 2, plan.wide, 2 * plan.crow
            steps = 8 * plan.h // wide
            total = keep_ref[...] + other_ref[...].astype(F32)
            for v in range(steps):
                for g in range(wide // LANES):
                    at = v * wide + g * LANES
                    scr_sum[g, pl.ds(v, half, stride=steps), :] = total[:, at : at + LANES]
            for d in range(plan.n):
                for g in range(wide // LANES):
                    at = plan.pos + g * LANES
                    x_ref[d, :, at : at + LANES] = scr_sum[g, per * d : per * (d + 1), :].astype(BF16)

    return body


def call(body, name, outs, args, scratch=(), scalars=0, far_in=0, after=0, far_out=()):
    near = pl.BlockSpec(memory_space=pltpu.VMEM)
    far = pl.BlockSpec(memory_space=pltpu.HBM)
    ins = [pl.BlockSpec(memory_space=pltpu.SMEM)] * scalars + [far] * far_in
    args = [
        pltpu.with_memory_space_constraint(a, pltpu.HBM) if scalars <= i < len(ins) else a for i, a in enumerate(args)
    ]
    ins += [pl.BlockSpec(memory_space=pl.ANY)] * after
    return pl.pallas_call(
        body,
        name=name,
        in_specs=ins + [near] * (len(args) - len(ins)),
        out_specs=[far if i in far_out else near for i in range(len(outs))],
        out_shape=[jax.ShapeDtypeStruct(shape, kind) for shape, kind in outs],
        scratch_shapes=[pltpu.VMEM(s, F32) if isinstance(s, tuple) else s for s in scratch],
        compiler_params=pltpu.CompilerParams(vmem_limit_bytes=16 * 1024 * 1024),
    )(*args)


def exchange(x):
    return lax.all_to_all(x, AXES, 0, 0)


def solution(mesh):
    def local(pair, cotangent, token_mask, w_in1, w_out1, w_in2, w_out2):
        rt, ct, c = pair.shape
        h = w_out1.shape[0]
        plan = Plan(mesh, (rt, ct), c, h)
        n, cpd, pos, tokens = plan.n, plan.cpd, plan.pos, plan.tokens
        idx = jnp.stack([lax.axis_index("row"), lax.axis_index("col")]).astype(jnp.int32)
        lanes = (c, pos)
        both = (n, 2 * cpd, pos)
        single = (n, cpd, pos)
        group = plan.lane_groups
        scr1 = (group, tokens * cpd, LANES)
        scr2 = (group, tokens * 2 * cpd, LANES)

        flat = (pos, c)
        dma = pltpu.SemaphoreType.DMA
        halves = (c // 2, 8 * h)
        swap = [(i, i ^ 1) for i in range(plan.cols)]

        lifts = (c, h)
        wide = (2 * h, pos)
        back = (c, 2 * h)
        chip = (plan.wide // LANES, 2 * c, LANES)

        x1, z, mask = call(
            first_kernel(plan), "first", [(both, BF16), (lanes, BF16), ((8, pos), F32)],
            [idx, pair.reshape(flat), token_mask.reshape(1, tokens), w_in1],
            [pltpu.VMEM(flat, BF16), pltpu.VMEM((1, tokens), jnp.int32), pltpu.VMEM((c, 5 * h), BF16), flat, dma((3,))],
            scalars=1, far_in=3,
        )
        y1 = exchange(x1)
        x2, lr1 = call(
            product_kernel(plan, True), "product_out", [(single, BF16), ((2 * cpd, tokens, tokens), BF16)],
            [y1], [scr2, scr1],
        )
        y2 = exchange(x2)
        x3, mid, gate1, vc2, gc2, vw2, gw2 = call(
            middle_kernel(plan), "middle",
            [(both, BF16), (lanes, BF16), (lanes, F32), (wide, BF16), (wide, BF16), (back, BF16), (back, BF16)],
            [z, y2, mask, w_in1, w_out1, w_in2], [(h, pos)],
        )
        y3 = exchange(x3)
        x4, lr2 = call(
            product_kernel(plan, False), "product_in", [(single, BF16), ((2 * cpd, tokens, tokens), BF16)],
            [y3], [scr2, scr1],
        )
        y4 = exchange(x4)
        x5, cot, dog2 = call(
            turn_kernel(plan), "turn", [(single, BF16), (lanes, BF16), (lanes, BF16)],
            [y4, mid, cotangent.reshape(flat), w_in2, w_out2], [(h, pos), flat],
        )
        y5 = exchange(x5)
        (x6,) = call(grad_kernel(plan, False), "grads_in", [(both, BF16)], [y5, lr2], [scr1, scr2])
        y6 = exchange(x6)
        x7, mid_grad = call(
            back_kernel(plan), "back", [(single, BF16), (lanes, BF16)],
            [y6, vc2, gc2, vw2, gw2, dog2, mid, cot, gate1, w_in2, w_out1, y2], [(h, pos), wide],
        )
        y7 = exchange(x7)
        updated, og2, gg2 = call(
            after_turn_kernel(plan), "after_turn", [(flat, BF16), ((h, c), F32), (lifts, F32)],
            [mid_grad, y4, mid, cot, dog2, w_in2, w_out2],
            [(h, pos), flat, pltpu.VMEM(flat, BF16), dma(())], after=1, far_out=(0,),
        )
        keep, send, dog1 = call(
            after_back_kernel(plan), "after_back", [(halves, F32), (halves, BF16), (lanes, BF16)],
            [idx, y6, vc2, gc2, mid, mid_grad, gate1, y2, z, og2, gg2, w_out1],
            [(h, pos), wide, (c, 8 * h)], scalars=1,
        )
        other = lax.ppermute(send, "col", swap)
        vc1, gc1, vw1, gw1 = call(
            before_back_kernel(plan), "before_back1", [(wide, BF16), (wide, BF16), (back, BF16), (back, BF16)],
            [dog1, z, mask, w_in1], after=1,
        )
        (x8,) = call(
            grad_kernel(plan, True), "grads_out", [((n, 2 * cpd, pos + plan.wide), BF16)],
            [vw1, y7, lr1, keep, other], [scr1, scr2, chip], after=1,
        )
        y8 = exchange(x8)
        (x9,) = call(
            last_kernel(plan), "last", [((n, cpd, 4 * h + 2 * plan.wide), BF16)], [y8, z, vc1, gc1], [wide]
        )
        y9 = exchange(x9)
        (x10,) = call(sum_kernel(plan), "sum", [((n, cpd, 4 * h), BF16)], [y9])
        y10 = exchange(x10)
        (own,) = call(half_kernel(plan), "half", [((n, cpd, 2 * plan.wide), BF16)], [y9])
        partner = lax.ppermute(own, "col", swap)
        (pair_grad,) = call(
            after_last_kernel(plan), "after_last", [(flat, BF16)],
            [y9, y8, z, mid_grad, dog1, vc1, gc1, vw1, gw1, w_in1],
            [wide, flat, pltpu.VMEM(flat, BF16), dma(())], after=1, far_out=(0,),
        )
        g1, out1, in2, out2 = call(
            assemble_kernel(plan), "assemble",
            [((c, h), F32), ((h, c), F32), ((c, 5 * h), F32), ((h, c), F32)],
            [idx, own, partner], [chip], scalars=1,
        )
        (in1,) = call(end_kernel(plan), "end", [((c, 5 * h), F32)], [y10, g1])
        return updated.reshape(rt, ct, c), pair_grad.reshape(rt, ct, c), in1, out1, in2, out2

    return jax.shard_map(
        local,
        mesh=mesh,
        in_specs=(P("row", "col", None), P("row", "col", None), P(), P(), P(), P(), P()),
        out_specs=(P("row", "col", None), P("row", "col", None), P(), P(), P(), P()),
        check_vma=False,
    )
```

```python
import jax
import jax.numpy as jnp
from jax import lax
from jax.experimental import pallas as pl
from jax.experimental.pallas import tpu as pltpu
from jax.sharding import PartitionSpec as P

EPSILON = 1e-05
LANES = 128
AXES = ("row", "col")
F32 = jnp.float32
BF16 = jnp.bfloat16


class Plan:
    def __init__(self, mesh, tile, width, hidden):
        self.rows = mesh.shape["row"]
        self.cols = mesh.shape["col"]
        self.n = self.rows * self.cols
        self.rt, self.ct = tile
        self.pos = self.rt * self.ct
        self.tokens = self.rt * self.rows
        self.c = width
        self.h = hidden
        self.cpd = hidden // self.n
        self.crow = width // self.n
        self.blocks = LANES // self.rt
        self.lane_groups = self.tokens // LANES
        self.seconds = self.pos // LANES
        self.wide = 8 * hidden // self.n * (width // 2) // (2 * self.crow)
        assert self.wide == 2 * hidden and self.cols % 2 == 0
        assert self.blocks >= 1 and self.cpd == self.crow
        assert self.rt & (self.rt - 1) == 0 and self.rows == self.blocks * self.lane_groups


def nn(a, b):
    return jnp.dot(a, b, preferred_element_type=F32)


def nt(a, b):
    return lax.dot_general(a, b, (((1,), (1,)), ((), ())), preferred_element_type=F32)


def iota(shape, axis):
    return lax.broadcasted_iota(jnp.int32, shape, axis)


def one_hot(cond):
    return jnp.where(cond, 1.0, 0.0).astype(BF16)


def eye(size):
    return one_hot(iota((size, size), 0) == iota((size, size), 1))


def to_lanes(tile_ref, scr, plan):
    scr[...] = tile_ref[...].astype(F32)
    rows = [scr[pl.ds(k, plan.rt, stride=plan.ct), :] for k in range(plan.ct)]
    return nt(eye(plan.c), jnp.concatenate(rows, axis=0).astype(BF16))


def from_lanes(lanes, scr, plan):
    turn = eye(LANES)
    for q in range(plan.seconds):
        block = nt(turn, lanes[:, q * LANES : (q + 1) * LANES])
        for b in range(plan.blocks):
            rows = block[b * plan.rt : (b + 1) * plan.rt, :]
            scr[pl.ds(q * plan.blocks + b, plan.rt, stride=plan.ct), :] = rows
    return scr[...].astype(BF16)


def split_order(plan):
    wide = 2 * plan.h
    row = iota((wide, wide), 0)
    source = iota((wide, wide), 1)
    per = 2 * plan.cpd
    bits = per.bit_length() - 1
    side = (row & (per - 1)) >> (bits - 1)
    channel = (row >> bits) * plan.cpd + (row & (plan.cpd - 1))
    return one_hot(source == side * plan.h + channel)


def sides(w, first, plan):
    h = plan.h
    return jnp.concatenate([w[:, first * h : (first + 1) * h], w[:, (first + 2) * h : (first + 3) * h]], axis=1)


def standard(x):
    centre = jnp.mean(x, axis=0, keepdims=True)
    shifted = x - centre
    spread = jnp.mean(shifted * shifted, axis=0, keepdims=True)
    scale = lax.rsqrt(spread + EPSILON)
    return shifted * scale, scale


def standard_grad(unit, scale, grad):
    flat = jnp.mean(grad, axis=0, keepdims=True)
    along = jnp.mean(grad * unit, axis=0, keepdims=True)
    return scale * (grad - flat - unit * along)


def split_weights(w, plan, perm=None):
    perm = split_order(plan) if perm is None else perm
    return nt(perm, sides(w, 0, plan)).astype(BF16), nt(perm, sides(w, 1, plan)).astype(BF16)


def split_projection(normed, value_w, gate_w):
    return nn(value_w, normed), jax.nn.sigmoid(nn(gate_w, normed))


def out_gate(normed, w, plan):
    tail = nt(eye(plan.h), w[:, 4 * plan.h :]).astype(BF16)
    return jax.nn.sigmoid(nn(tail, normed))


def back_coefficients(normed, w, mask, plan):
    value, gate = split_projection(normed, *split_weights(w, plan))
    through = gate * mask
    return through, through * value * (1.0 - gate)


def back_weights(w, plan):
    perm = split_order(plan)
    return nt(sides(w, 0, plan), perm).astype(BF16), nt(sides(w, 1, plan), perm).astype(BF16)


def side_terms(normed, value_grad, gate_grad, plan):
    perm = split_order(plan)
    value_part = nn(nt(normed, value_grad).astype(BF16), perm)
    gate_part = nn(nt(normed, gate_grad).astype(BF16), perm)
    h = plan.h
    return [value_part[:, :h], gate_part[:, :h], value_part[:, h:], gate_part[:, h:]]


def put_rows(dest_ref, value, per, plan, start=0):
    size = value.shape[1]
    for d in range(plan.n):
        dest_ref[d, :, start : start + size] = value[per * d : per * (d + 1), :].astype(dest_ref.dtype)


def get_rows(source_ref, scratch_ref, per, plan, start, size):
    if per % 8 == 0:
        rows = [source_ref[d, :, start : start + size].astype(F32) for d in range(plan.n)]
        return jnp.concatenate(rows, axis=0)
    for d in range(plan.n):
        scratch_ref[per * d : per * (d + 1), :size] = source_ref[d, :, start : start + size].astype(F32)
    return scratch_ref[:, :size]


def first_kernel(plan):
    def body(idx, pair_hbm, tokens_hbm, w_hbm, x_ref, z_ref, mask_ref, pair, tokens, w_in, scr, sems):
        sources = (pair_hbm, tokens_hbm, w_hbm)
        copies = [
            pltpu.make_async_copy(source, dest, sems.at[i])
            for i, (source, dest) in enumerate(zip(sources, (pair, tokens, w_in)))
        ]
        for copy in copies:
            copy.start()
        token = iota((plan.tokens, plan.pos), 0)
        lane = iota((plan.tokens, plan.pos), 1)
        shift = plan.rt.bit_length() - 1
        first = one_hot(token == idx[0] * plan.rt + (lane & (plan.rt - 1)))
        second = one_hot(token == idx[1] * plan.ct + (lane >> shift))
        perm = split_order(plan)
        for copy in copies:
            copy.wait()
        flags = jnp.broadcast_to(tokens[...].astype(F32), (8, plan.tokens)).astype(BF16)
        mask = nn(flags, first) * nn(flags, second)
        mask_ref[...] = mask
        z = to_lanes(pair, scr, plan)
        z_ref[...] = z.astype(BF16)
        value_w, gate_w = split_weights(w_in[...], plan, perm)
        value, gate = split_projection(standard(z)[0].astype(BF16), value_w, gate_w)
        put_rows(x_ref, gate * value * mask[:1], 2 * plan.cpd, plan)

    return body


def middle_kernel(plan):
    def body(z_ref, y_ref, mask_ref, w_in1, w_out1, w_in2, x_ref, mid_ref, gate_out, vc_ref, gc_ref, vw_ref, gw_ref, scr):
        z = z_ref[...].astype(F32)
        gate = out_gate(standard(z)[0].astype(BF16), w_in1[...], plan)
        gate_out[...] = gate
        tri = get_rows(y_ref, scr, plan.cpd, plan, 0, plan.pos)
        lifted = nn(nt(eye(plan.c), w_out1[...]).astype(BF16), standard(tri)[0].astype(BF16))
        mid = (z + gate * lifted).astype(BF16)
        mid_ref[...] = mid
        normed = standard(mid.astype(F32))[0].astype(BF16)
        value, gate = split_projection(normed, *split_weights(w_in2[...], plan))
        through = gate * mask_ref[:1, :]
        part = through * value
        put_rows(x_ref, part, 2 * plan.cpd, plan)
        vc_ref[...] = through.astype(BF16)
        gc_ref[...] = (part * (1.0 - gate)).astype(BF16)
        vw_ref[...], gw_ref[...] = back_weights(w_in2[...], plan)

    return body


def turn_kernel(plan):
    def body(y_ref, mid_ref, cot_ref, w_in2, w_out2, x_ref, cot_out, dog_ref, scr, flat):
        cot = to_lanes(cot_ref, flat, plan)
        cot_out[...] = cot.astype(BF16)
        gate = out_gate(standard(mid_ref[...].astype(F32))[0].astype(BF16), w_in2[...], plan)
        lift_grad = (gate * cot).astype(BF16)
        unit, scale = standard(get_rows(y_ref, scr, plan.cpd, plan, 0, plan.pos))
        put_rows(x_ref, standard_grad(unit, scale, nn(w_out2[...], lift_grad)), plan.cpd, plan)
        lifted = nn(nt(eye(plan.c), w_out2[...]).astype(BF16), unit.astype(BF16))
        dog_ref[...] = (lifted * cot * gate * (1.0 - gate)).astype(BF16)

    return body


def after_turn_kernel(plan):
    def body(after, y_ref, mid_ref, cot_ref, dog_ref, w_in2, w_out2, up_hbm, og_ref, gg_ref, scr, flat, up, sem):
        tri = get_rows(y_ref, scr, plan.cpd, plan, 0, plan.pos)
        rounded = standard(tri)[0].astype(BF16)
        lifted = nn(nt(eye(plan.c), w_out2[...]).astype(BF16), rounded)
        mid, cot = mid_ref[...].astype(F32), cot_ref[...].astype(F32)
        normed = standard(mid)[0].astype(BF16)
        gate = out_gate(normed, w_in2[...], plan)
        up[...] = from_lanes((mid + gate * lifted).astype(BF16), flat, plan)
        copy = pltpu.make_async_copy(up, up_hbm, sem)
        copy.start()
        og_ref[...] = nt(rounded, (gate * cot).astype(BF16))
        gg_ref[...] = nt(normed, dog_ref[...])
        copy.wait()

    return body


def before_back_kernel(plan):
    def body(after, source_ref, mask_ref, w_in, vc_ref, gc_ref, vw_ref, gw_ref):
        normed = standard(source_ref[...].astype(F32))[0].astype(BF16)
        value, gate = back_coefficients(normed, w_in[...], mask_ref[:1, :], plan)
        vc_ref[...] = value.astype(BF16)
        gc_ref[...] = gate.astype(BF16)
        vw_ref[...], gw_ref[...] = back_weights(w_in[...], plan)

    return body


def side_grads(y_ref, vc_ref, gc_ref, scr, plan):
    grad = get_rows(y_ref, scr, 2 * plan.cpd, plan, 0, plan.pos)
    return (grad * vc_ref[...].astype(F32)).astype(BF16), (grad * gc_ref[...].astype(F32)).astype(BF16)


def back_kernel(plan):
    def body(y6, vc_ref, gc_ref, vw_ref, gw_ref, dog_ref, mid_ref, cot_ref, gate_ref, w_in2, w_out1, y2,
             x_ref, mg_ref, scr, scr2):
        value_grad, gate_grad = side_grads(y6, vc_ref, gc_ref, scr2, plan)
        normed_grad = nn(vw_ref[...], value_grad) + nn(gw_ref[...], gate_grad)
        normed_grad += nn(w_in2[:, 4 * plan.h :], dog_ref[...])
        unit, scale = standard(mid_ref[...].astype(F32))
        mid_grad = (cot_ref[...].astype(F32) + standard_grad(unit, scale, normed_grad)).astype(BF16)
        mg_ref[...] = mid_grad
        lift_grad = (gate_ref[...] * mid_grad.astype(F32)).astype(BF16)
        unit, scale = standard(get_rows(y2, scr, plan.cpd, plan, 0, plan.pos))
        put_rows(x_ref, standard_grad(unit, scale, nn(w_out1[...], lift_grad)), plan.cpd, plan)

    return body


def after_back_kernel(plan):
    def body(idx, y6, vc_ref, gc_ref, mid_ref, mg_ref, gate_ref, y2, z_ref, og2, gg2, w_out1,
             keep_ref, send_ref, dog_ref, scr, scr2, sums):
        value_grad, gate_grad = side_grads(y6, vc_ref, gc_ref, scr2, plan)
        terms = side_terms(standard(mid_ref[...].astype(F32))[0].astype(BF16), value_grad, gate_grad, plan)
        mid_grad, gate = mg_ref[...].astype(F32), gate_ref[...]
        lift_grad = (gate * mid_grad).astype(BF16)
        rounded = standard(get_rows(y2, scr, plan.cpd, plan, 0, plan.pos))[0].astype(BF16)
        lifted = nn(nt(eye(plan.c), w_out1[...]).astype(BF16), rounded)
        dog = (lifted * mid_grad * gate * (1.0 - gate)).astype(BF16)
        dog_ref[...] = dog
        normed = standard(z_ref[...].astype(F32))[0].astype(BF16)
        terms += [gg2[...], og2[...], nt(rounded, lift_grad), nt(normed, dog)]
        at = 0
        for part in terms:
            sums[:, at : at + part.shape[1]] = part
            at += part.shape[1]
        half = plan.c // 2
        core = idx[1] & 1
        keep_ref[...] = sums[pl.ds(pl.multiple_of(core * half, 8), half), :]
        send_ref[...] = sums[pl.ds(pl.multiple_of((1 - core) * half, 8), half), :].astype(BF16)

    return body


def last_kernel(plan):
    def body(y8, z_ref, vc_ref, gc_ref, x_ref, scr):
        wide, per = plan.wide, 2 * plan.crow
        value_grad, gate_grad = side_grads(y8, vc_ref, gc_ref, scr, plan)
        normed = standard(z_ref[...].astype(F32))[0].astype(BF16)
        terms = jnp.concatenate(side_terms(normed, value_grad, gate_grad, plan), axis=1)
        totals = []
        for core in range(2):
            total = y8[core, :, plan.pos :].astype(F32)
            for d in range(core + 2, plan.n, 2):
                total = total + y8[d, :, plan.pos :].astype(F32)
            totals.append((total * (1.0 / plan.tokens)).astype(BF16))
        for d in range(plan.n):
            rows = slice(per * (d // 2), per * (d // 2 + 1))
            x_ref[d, :, :wide] = terms[rows, wide * (d % 2) : wide * (d % 2 + 1)].astype(BF16)
            x_ref[d, :, wide:] = totals[d % 2]

    return body


def after_last_kernel(plan):
    def body(after, y8, z_ref, mg_ref, dog_ref, vc_ref, gc_ref, vw_ref, gw_ref, w_in1, pg_hbm, scr, flat, pg, sem):
        value_grad, gate_grad = side_grads(y8, vc_ref, gc_ref, scr, plan)
        normed_grad = nn(vw_ref[...], value_grad) + nn(gw_ref[...], gate_grad)
        normed_grad += nn(w_in1[:, 4 * plan.h :], dog_ref[...])
        unit, scale = standard(z_ref[...].astype(F32))
        grad = mg_ref[...].astype(F32) + standard_grad(unit, scale, normed_grad)
        pg[...] = from_lanes(grad.astype(BF16), flat, plan)
        copy = pltpu.make_async_copy(pg, pg_hbm, sem)
        copy.start()
        copy.wait()

    return body


def sum_kernel(plan):
    def body(y_ref, x_ref):
        total = y_ref[0, :, : plan.wide].astype(F32)
        for d in range(1, plan.n):
            total = total + y_ref[d, :, : plan.wide].astype(F32)
        total = (total * (1.0 / plan.tokens)).astype(BF16)
        for d in range(plan.n):
            x_ref[d] = total

    return body


def half_kernel(plan):
    def body(y_ref, half_ref):
        half_ref[...] = y_ref[:, :, plan.wide :]

    return body


def assemble_kernel(plan):
    def body(idx, own_ref, other_ref, g1_ref, out1_ref, in2_ref, out2_ref, scr):
        h, wide, per = plan.h, plan.wide, 2 * plan.crow
        half = plan.c // 2
        steps = 8 * h // wide
        outs = ((in2_ref, 5 * h), (out2_ref, h), (out1_ref, h), (g1_ref, h))
        for k, ref in enumerate((own_ref, other_ref)):
            for d in range(plan.n):
                for g in range(wide // LANES):
                    scr[g, per * d : per * (d + 1), :] = ref[d, :, g * LANES : (g + 1) * LANES].astype(F32)
            core = idx[1] & 1 if k == 0 else 1 - (idx[1] & 1)
            rows = pl.ds(pl.multiple_of(core * half, 8), half)
            pieces = [
                scr[g, pl.ds(v, half, stride=steps), :] for v in range(steps) for g in range(wide // LANES)
            ]
            for out_ref, size in outs:
                for i in range(size // LANES):
                    out_ref[rows, i * LANES : (i + 1) * LANES] = pieces.pop(0)

    return body


def end_kernel(plan):
    def body(y_ref, g1_ref, in1_ref):
        wide, per = plan.wide, 2 * plan.crow
        for d in range(plan.n):
            rows = slice(per * (d // 2), per * (d // 2 + 1))
            in1_ref[rows, wide * (d % 2) : wide * (d % 2 + 1)] = y_ref[d].astype(F32)
        in1_ref[:, 2 * wide :] = g1_ref[...]

    return body


def turn_blocks(group, plan):
    count, size = plan.blocks, plan.rt
    lane = iota(group[0].shape, 1)
    group = list(group)
    step = count // 2
    while step:
        low = (lane & (step * size)) == 0
        for a in range(count):
            if a & step == 0:
                x, y = group[a], group[a + step]
                group[a] = jnp.where(low, x, pltpu.roll(y, step * size, 1))
                group[a + step] = jnp.where(low, pltpu.roll(x, LANES - step * size, 1), y)
        step //= 2
    return group


def spread(y_ref, scr, per, plan, steps=1):
    def column(c, carry):
        for g in range(plan.lane_groups):
            for q in range(plan.seconds):
                group = []
                for b in range(plan.blocks):
                    src = (g * plan.blocks + b) * plan.cols + c
                    group.append(y_ref[src, :per, q * LANES : (q + 1) * LANES].astype(F32))
                group = turn_blocks(group, plan)
                for b in range(plan.blocks):
                    row = pl.multiple_of((c * plan.ct + q * plan.blocks + b) * per, per)
                    scr[g, pl.ds(row, per), :] = group[b]
        return carry

    lax.fori_loop(0, plan.cols, column, 0, unroll=plan.cols // steps)


def collect(scr, x_ref, per, plan):
    def column(c, carry):
        for g in range(plan.lane_groups):
            for q in range(plan.seconds):
                group = []
                for b in range(plan.blocks):
                    row = pl.multiple_of((c * plan.ct + q * plan.blocks + b) * per, per)
                    group.append(scr[g, pl.ds(row, per), :])
                group = turn_blocks(group, plan)
                for b in range(plan.blocks):
                    dest = (g * plan.blocks + b) * plan.cols + c
                    x_ref[dest, :per, q * LANES : (q + 1) * LANES] = group[b].astype(BF16)
        return carry

    lax.fori_loop(0, plan.cols, column, 0, unroll=plan.cols)


def pick(scr, row, per, plan):
    parts = [scr[g, pl.ds(row, plan.tokens, stride=per), :] for g in range(plan.lane_groups)]
    return parts[0] if len(parts) == 1 else jnp.concatenate(parts, axis=1)


def place(scr, row, per, value, plan):
    for g in range(plan.lane_groups):
        scr[g, pl.ds(row, plan.tokens, stride=per), :] = value[:, g * LANES : (g + 1) * LANES]


def product_kernel(plan, outgoing):
    cpd = plan.cpd

    def body(y_ref, x_ref, lr_ref, scr, scr_out):
        turn = eye(plan.tokens)
        spread(y_ref, scr, 2 * cpd, plan, 1 if outgoing else 2)
        sides = [pick(scr, row, 2 * cpd, plan).astype(BF16) for row in range(2 * cpd)]
        for row, side in enumerate(sides):
            lr_ref[row] = side
        left, right = sides[:cpd], sides[cpd:]
        if outgoing:
            right = [nt(turn, side).astype(BF16) for side in right]
        for t, tri in enumerate([nn(b, a) if outgoing else nt(b, a) for a, b in zip(left, right)]):
            place(scr_out, t, cpd, tri, plan)
        collect(scr_out, x_ref, cpd, plan)

    return body


def grad_kernel(plan, outgoing):
    cpd = plan.cpd

    def body(*refs):
        if outgoing:
            after, y_ref, lr_ref, keep_ref, other_ref, x_ref, scr, scr_out, scr_sum = refs
        else:
            y_ref, lr_ref, x_ref, scr, scr_out = refs
        turn = eye(plan.tokens)
        spread(y_ref, scr, cpd, plan, 2 if outgoing else 1)
        left = [lr_ref[t] for t in range(cpd)]
        right = [lr_ref[cpd + t] for t in range(cpd)]
        grads = [pick(scr, t, cpd, plan).astype(BF16) for t in range(cpd)]
        if outgoing:
            terms = [nn(b, grad) for b, grad in zip(right, grads)] + [nt(a, grad) for a, grad in zip(left, grads)]
        else:
            turned = [nt(turn, grad).astype(BF16) for grad in grads]
            terms = [nn(grad, b) for b, grad in zip(right, turned)] + [nn(grad, a) for a, grad in zip(left, grads)]
        for row, term in enumerate(terms):
            place(scr_out, row, 2 * cpd, term, plan)
        collect(scr_out, x_ref, 2 * cpd, plan)
        if outgoing:
            half, wide, per = plan.c // 2, plan.wide, 2 * plan.crow
            steps = 8 * plan.h // wide
            total = keep_ref[...] + other_ref[...].astype(F32)
            for v in range(steps):
                for g in range(wide // LANES):
                    at = v * wide + g * LANES
                    scr_sum[g, pl.ds(v, half, stride=steps), :] = total[:, at : at + LANES]
            for d in range(plan.n):
                for g in range(wide // LANES):
                    at = plan.pos + g * LANES
                    x_ref[d, :, at : at + LANES] = scr_sum[g, per * d : per * (d + 1), :].astype(BF16)

    return body


def call(body, name, outs, args, scratch=(), scalars=0, far_in=0, after=0, far_out=()):
    near = pl.BlockSpec(memory_space=pltpu.VMEM)
    far = pl.BlockSpec(memory_space=pltpu.HBM)
    ins = [pl.BlockSpec(memory_space=pltpu.SMEM)] * scalars + [far] * far_in
    args = [
        pltpu.with_memory_space_constraint(a, pltpu.HBM) if scalars <= i < len(ins) else a for i, a in enumerate(args)
    ]
    ins += [pl.BlockSpec(memory_space=pl.ANY)] * after
    return pl.pallas_call(
        body,
        name=name,
        in_specs=ins + [near] * (len(args) - len(ins)),
        out_specs=[far if i in far_out else near for i in range(len(outs))],
        out_shape=[jax.ShapeDtypeStruct(shape, kind) for shape, kind in outs],
        scratch_shapes=[pltpu.VMEM(s, F32) if isinstance(s, tuple) else s for s in scratch],
        compiler_params=pltpu.CompilerParams(vmem_limit_bytes=16 * 1024 * 1024),
    )(*args)


def exchange(x):
    return lax.all_to_all(x, AXES, 0, 0)


def solution(mesh):
    def local(pair, cotangent, token_mask, w_in1, w_out1, w_in2, w_out2):
        rt, ct, c = pair.shape
        h = w_out1.shape[0]
        plan = Plan(mesh, (rt, ct), c, h)
        n, cpd, pos, tokens = plan.n, plan.cpd, plan.pos, plan.tokens
        idx = jnp.stack([lax.axis_index("row"), lax.axis_index("col")]).astype(jnp.int32)
        lanes = (c, pos)
        both = (n, 2 * cpd, pos)
        single = (n, cpd, pos)
        group = plan.lane_groups
        scr1 = (group, tokens * cpd, LANES)
        scr2 = (group, tokens * 2 * cpd, LANES)

        flat = (pos, c)
        dma = pltpu.SemaphoreType.DMA
        halves = (c // 2, 8 * h)
        swap = [(i, i ^ 1) for i in range(plan.cols)]

        lifts = (c, h)
        wide = (2 * h, pos)
        back = (c, 2 * h)
        chip = (plan.wide // LANES, 2 * c, LANES)

        x1, z, mask = call(
            first_kernel(plan), "first", [(both, BF16), (lanes, BF16), ((8, pos), F32)],
            [idx, pair.reshape(flat), token_mask.reshape(1, tokens), w_in1],
            [pltpu.VMEM(flat, BF16), pltpu.VMEM((1, tokens), jnp.int32), pltpu.VMEM((c, 5 * h), BF16), flat, dma((3,))],
            scalars=1, far_in=3,
        )
        y1 = exchange(x1)
        x2, lr1 = call(
            product_kernel(plan, True), "product_out", [(single, BF16), ((2 * cpd, tokens, tokens), BF16)],
            [y1], [scr2, scr1],
        )
        y2 = exchange(x2)
        x3, mid, gate1, vc2, gc2, vw2, gw2 = call(
            middle_kernel(plan), "middle",
            [(both, BF16), (lanes, BF16), (lanes, F32), (wide, BF16), (wide, BF16), (back, BF16), (back, BF16)],
            [z, y2, mask, w_in1, w_out1, w_in2], [(h, pos)],
        )
        y3 = exchange(x3)
        x4, lr2 = call(
            product_kernel(plan, False), "product_in", [(single, BF16), ((2 * cpd, tokens, tokens), BF16)],
            [y3], [scr2, scr1],
        )
        y4 = exchange(x4)
        x5, cot, dog2 = call(
            turn_kernel(plan), "turn", [(single, BF16), (lanes, BF16), (lanes, BF16)],
            [y4, mid, cotangent.reshape(flat), w_in2, w_out2], [(h, pos), flat],
        )
        y5 = exchange(x5)
        (x6,) = call(grad_kernel(plan, False), "grads_in", [(both, BF16)], [y5, lr2], [scr1, scr2])
        y6 = exchange(x6)
        x7, mid_grad = call(
            back_kernel(plan), "back", [(single, BF16), (lanes, BF16)],
            [y6, vc2, gc2, vw2, gw2, dog2, mid, cot, gate1, w_in2, w_out1, y2], [(h, pos), wide],
        )
        y7 = exchange(x7)
        updated, og2, gg2 = call(
            after_turn_kernel(plan), "after_turn", [(flat, BF16), ((h, c), F32), (lifts, F32)],
            [mid_grad, y4, mid, cot, dog2, w_in2, w_out2],
            [(h, pos), flat, pltpu.VMEM(flat, BF16), dma(())], after=1, far_out=(0,),
        )
        keep, send, dog1 = call(
            after_back_kernel(plan), "after_back", [(halves, F32), (halves, BF16), (lanes, BF16)],
            [idx, y6, vc2, gc2, mid, mid_grad, gate1, y2, z, og2, gg2, w_out1],
            [(h, pos), wide, (c, 8 * h)], scalars=1,
        )
        other = lax.ppermute(send, "col", swap)
        vc1, gc1, vw1, gw1 = call(
            before_back_kernel(plan), "before_back1", [(wide, BF16), (wide, BF16), (back, BF16), (back, BF16)],
            [dog1, z, mask, w_in1], after=1,
        )
        (x8,) = call(
            grad_kernel(plan, True), "grads_out", [((n, 2 * cpd, pos + plan.wide), BF16)],
            [vw1, y7, lr1, keep, other], [scr1, scr2, chip], after=1,
        )
        y8 = exchange(x8)
        (x9,) = call(
            last_kernel(plan), "last", [((n, 2 * cpd, 2 * plan.wide), BF16)], [y8, z, vc1, gc1], [wide]
        )
        y9 = exchange(x9)
        (x10,) = call(sum_kernel(plan), "sum", [((n, 2 * cpd, plan.wide), BF16)], [y9])
        y10 = exchange(x10)
        (own,) = call(half_kernel(plan), "half", [((n, 2 * cpd, plan.wide), BF16)], [y9])
        partner = lax.ppermute(own, "col", swap)
        (pair_grad,) = call(
            after_last_kernel(plan), "after_last", [(flat, BF16)],
            [y9, y8, z, mid_grad, dog1, vc1, gc1, vw1, gw1, w_in1],
            [wide, flat, pltpu.VMEM(flat, BF16), dma(())], after=1, far_out=(0,),
        )
        g1, out1, in2, out2 = call(
            assemble_kernel(plan), "assemble",
            [((c, h), F32), ((h, c), F32), ((c, 5 * h), F32), ((h, c), F32)],
            [idx, own, partner], [chip], scalars=1,
        )
        (in1,) = call(end_kernel(plan), "end", [((c, 5 * h), F32)], [y10, g1])
        return updated.reshape(rt, ct, c), pair_grad.reshape(rt, ct, c), in1, out1, in2, out2

    return jax.shard_map(
        local,
        mesh=mesh,
        in_specs=(P("row", "col", None), P("row", "col", None), P(), P(), P(), P(), P()),
        out_specs=(P("row", "col", None), P("row", "col", None), P(), P(), P(), P()),
        check_vma=False,
    )
```

```python
import jax
import jax.numpy as jnp
from jax import lax
from jax.experimental import pallas as pl
from jax.experimental.pallas import tpu as pltpu
from jax.sharding import PartitionSpec as P

EPSILON = 1e-05
LANES = 128
AXES = ("row", "col")
F32 = jnp.float32
BF16 = jnp.bfloat16


class Plan:
    def __init__(self, mesh, tile, width, hidden):
        self.rows = mesh.shape["row"]
        self.cols = mesh.shape["col"]
        self.n = self.rows * self.cols
        self.rt, self.ct = tile
        self.pos = self.rt * self.ct
        self.tokens = self.rt * self.rows
        self.c = width
        self.h = hidden
        self.cpd = hidden // self.n
        self.crow = width // self.n
        self.blocks = LANES // self.rt
        self.lane_groups = self.tokens // LANES
        self.seconds = self.pos // LANES
        self.wide = 8 * hidden // self.n * (width // 2) // (2 * self.crow)
        self.quarter = self.wide // 2
        assert self.wide == 2 * hidden and self.quarter == LANES
        assert self.cols % 2 == 0 and self.rows % 2 == 0
        assert self.blocks >= 1 and self.cpd == self.crow
        assert self.rt & (self.rt - 1) == 0 and self.rows == self.blocks * self.lane_groups


def nn(a, b):
    return jnp.dot(a, b, preferred_element_type=F32)


def nt(a, b):
    return lax.dot_general(a, b, (((1,), (1,)), ((), ())), preferred_element_type=F32)


def iota(shape, axis):
    return lax.broadcasted_iota(jnp.int32, shape, axis)


def one_hot(cond):
    return jnp.where(cond, 1.0, 0.0).astype(BF16)


def eye(size):
    return one_hot(iota((size, size), 0) == iota((size, size), 1))


def to_lanes(tile_ref, scr, plan):
    scr[...] = tile_ref[...].astype(F32)
    rows = [scr[pl.ds(k, plan.rt, stride=plan.ct), :] for k in range(plan.ct)]
    return nt(eye(plan.c), jnp.concatenate(rows, axis=0).astype(BF16))


def from_lanes(lanes, scr, plan):
    turn = eye(LANES)
    for q in range(plan.seconds):
        block = nt(turn, lanes[:, q * LANES : (q + 1) * LANES])
        for b in range(plan.blocks):
            rows = block[b * plan.rt : (b + 1) * plan.rt, :]
            scr[pl.ds(q * plan.blocks + b, plan.rt, stride=plan.ct), :] = rows
    return scr[...].astype(BF16)


def split_order(plan):
    wide = 2 * plan.h
    row = iota((wide, wide), 0)
    source = iota((wide, wide), 1)
    per = 2 * plan.cpd
    bits = per.bit_length() - 1
    side = (row & (per - 1)) >> (bits - 1)
    channel = (row >> bits) * plan.cpd + (row & (plan.cpd - 1))
    return one_hot(source == side * plan.h + channel)


def sides(w, first, plan):
    h = plan.h
    return jnp.concatenate([w[:, first * h : (first + 1) * h], w[:, (first + 2) * h : (first + 3) * h]], axis=1)


def standard(x):
    centre = jnp.mean(x, axis=0, keepdims=True)
    shifted = x - centre
    spread = jnp.mean(shifted * shifted, axis=0, keepdims=True)
    scale = lax.rsqrt(spread + EPSILON)
    return shifted * scale, scale


def standard_grad(unit, scale, grad):
    flat = jnp.mean(grad, axis=0, keepdims=True)
    along = jnp.mean(grad * unit, axis=0, keepdims=True)
    return scale * (grad - flat - unit * along)


def split_weights(w, plan, perm=None):
    perm = split_order(plan) if perm is None else perm
    return nt(perm, sides(w, 0, plan)).astype(BF16), nt(perm, sides(w, 1, plan)).astype(BF16)


def split_projection(normed, value_w, gate_w):
    return nn(value_w, normed), jax.nn.sigmoid(nn(gate_w, normed))


def out_gate(normed, w, plan):
    tail = nt(eye(plan.h), w[:, 4 * plan.h :]).astype(BF16)
    return jax.nn.sigmoid(nn(tail, normed))


def back_coefficients(normed, w, mask, plan):
    value, gate = split_projection(normed, *split_weights(w, plan))
    through = gate * mask
    return through, through * value * (1.0 - gate)


def back_weights(w, plan):
    perm = split_order(plan)
    return nt(sides(w, 0, plan), perm).astype(BF16), nt(sides(w, 1, plan), perm).astype(BF16)


def side_terms(normed, value_grad, gate_grad, plan):
    perm = split_order(plan)
    value_part = nn(nt(normed, value_grad).astype(BF16), perm)
    gate_part = nn(nt(normed, gate_grad).astype(BF16), perm)
    h = plan.h
    return [value_part[:, :h], gate_part[:, :h], value_part[:, h:], gate_part[:, h:]]


def put_rows(dest_ref, value, per, plan, start=0):
    size = value.shape[1]
    for d in range(plan.n):
        dest_ref[d, :, start : start + size] = value[per * d : per * (d + 1), :].astype(dest_ref.dtype)


def get_rows(source_ref, scratch_ref, per, plan, start, size):
    if per % 8 == 0:
        rows = [source_ref[d, :, start : start + size].astype(F32) for d in range(plan.n)]
        return jnp.concatenate(rows, axis=0)
    for d in range(plan.n):
        scratch_ref[per * d : per * (d + 1), :size] = source_ref[d, :, start : start + size].astype(F32)
    return scratch_ref[:, :size]


def first_kernel(plan):
    def body(idx, pair_hbm, tokens_hbm, w_hbm, x_ref, z_ref, mask_ref, pair, tokens, w_in, scr, sems):
        sources = (pair_hbm, tokens_hbm, w_hbm)
        copies = [
            pltpu.make_async_copy(source, dest, sems.at[i])
            for i, (source, dest) in enumerate(zip(sources, (pair, tokens, w_in)))
        ]
        for copy in copies:
            copy.start()
        token = iota((plan.tokens, plan.pos), 0)
        lane = iota((plan.tokens, plan.pos), 1)
        shift = plan.rt.bit_length() - 1
        first = one_hot(token == idx[0] * plan.rt + (lane & (plan.rt - 1)))
        second = one_hot(token == idx[1] * plan.ct + (lane >> shift))
        perm = split_order(plan)
        for copy in copies:
            copy.wait()
        flags = jnp.broadcast_to(tokens[...].astype(F32), (8, plan.tokens)).astype(BF16)
        mask = nn(flags, first) * nn(flags, second)
        mask_ref[...] = mask
        z = to_lanes(pair, scr, plan)
        z_ref[...] = z.astype(BF16)
        value_w, gate_w = split_weights(w_in[...], plan, perm)
        value, gate = split_projection(standard(z)[0].astype(BF16), value_w, gate_w)
        put_rows(x_ref, gate * value * mask[:1], 2 * plan.cpd, plan)

    return body


def middle_kernel(plan):
    def body(z_ref, y_ref, mask_ref, w_in1, w_out1, w_in2, x_ref, mid_ref, gate_out, vc_ref, gc_ref, vw_ref, gw_ref, scr):
        z = z_ref[...].astype(F32)
        gate = out_gate(standard(z)[0].astype(BF16), w_in1[...], plan)
        gate_out[...] = gate
        tri = get_rows(y_ref, scr, plan.cpd, plan, 0, plan.pos)
        lifted = nn(nt(eye(plan.c), w_out1[...]).astype(BF16), standard(tri)[0].astype(BF16))
        mid = (z + gate * lifted).astype(BF16)
        mid_ref[...] = mid
        normed = standard(mid.astype(F32))[0].astype(BF16)
        value, gate = split_projection(normed, *split_weights(w_in2[...], plan))
        through = gate * mask_ref[:1, :]
        part = through * value
        put_rows(x_ref, part, 2 * plan.cpd, plan)
        vc_ref[...] = through.astype(BF16)
        gc_ref[...] = (part * (1.0 - gate)).astype(BF16)
        vw_ref[...], gw_ref[...] = back_weights(w_in2[...], plan)

    return body


def turn_kernel(plan):
    def body(y_ref, mid_ref, cot_ref, w_in2, w_out2, x_ref, cot_out, dog_ref, scr, flat):
        cot = to_lanes(cot_ref, flat, plan)
        cot_out[...] = cot.astype(BF16)
        gate = out_gate(standard(mid_ref[...].astype(F32))[0].astype(BF16), w_in2[...], plan)
        lift_grad = (gate * cot).astype(BF16)
        unit, scale = standard(get_rows(y_ref, scr, plan.cpd, plan, 0, plan.pos))
        put_rows(x_ref, standard_grad(unit, scale, nn(w_out2[...], lift_grad)), plan.cpd, plan)
        lifted = nn(nt(eye(plan.c), w_out2[...]).astype(BF16), unit.astype(BF16))
        dog_ref[...] = (lifted * cot * gate * (1.0 - gate)).astype(BF16)

    return body


def after_turn_kernel(plan):
    def body(after, y_ref, mid_ref, cot_ref, dog_ref, w_in2, w_out2, up_hbm, og_ref, gg_ref, scr, flat, up, sem):
        tri = get_rows(y_ref, scr, plan.cpd, plan, 0, plan.pos)
        rounded = standard(tri)[0].astype(BF16)
        lifted = nn(nt(eye(plan.c), w_out2[...]).astype(BF16), rounded)
        mid, cot = mid_ref[...].astype(F32), cot_ref[...].astype(F32)
        normed = standard(mid)[0].astype(BF16)
        gate = out_gate(normed, w_in2[...], plan)
        up[...] = from_lanes((mid + gate * lifted).astype(BF16), flat, plan)
        copy = pltpu.make_async_copy(up, up_hbm, sem)
        copy.start()
        og_ref[...] = nt(rounded, (gate * cot).astype(BF16))
        gg_ref[...] = nt(normed, dog_ref[...])
        copy.wait()

    return body


def before_back_kernel(plan):
    def body(after, source_ref, mask_ref, w_in, vc_ref, gc_ref, vw_ref, gw_ref):
        normed = standard(source_ref[...].astype(F32))[0].astype(BF16)
        value, gate = back_coefficients(normed, w_in[...], mask_ref[:1, :], plan)
        vc_ref[...] = value.astype(BF16)
        gc_ref[...] = gate.astype(BF16)
        vw_ref[...], gw_ref[...] = back_weights(w_in[...], plan)

    return body


def side_grads(y_ref, vc_ref, gc_ref, scr, plan):
    grad = get_rows(y_ref, scr, 2 * plan.cpd, plan, 0, plan.pos)
    return (grad * vc_ref[...].astype(F32)).astype(BF16), (grad * gc_ref[...].astype(F32)).astype(BF16)


def back_kernel(plan):
    def body(y6, vc_ref, gc_ref, vw_ref, gw_ref, dog_ref, mid_ref, cot_ref, gate_ref, w_in2, w_out1, y2,
             x_ref, mg_ref, scr, scr2):
        value_grad, gate_grad = side_grads(y6, vc_ref, gc_ref, scr2, plan)
        normed_grad = nn(vw_ref[...], value_grad) + nn(gw_ref[...], gate_grad)
        normed_grad += nn(w_in2[:, 4 * plan.h :], dog_ref[...])
        unit, scale = standard(mid_ref[...].astype(F32))
        mid_grad = (cot_ref[...].astype(F32) + standard_grad(unit, scale, normed_grad)).astype(BF16)
        mg_ref[...] = mid_grad
        lift_grad = (gate_ref[...] * mid_grad.astype(F32)).astype(BF16)
        unit, scale = standard(get_rows(y2, scr, plan.cpd, plan, 0, plan.pos))
        put_rows(x_ref, standard_grad(unit, scale, nn(w_out1[...], lift_grad)), plan.cpd, plan)

    return body


def after_back_kernel(plan):
    def body(idx, y6, vc_ref, gc_ref, mid_ref, mg_ref, gate_ref, y2, z_ref, og2, gg2, w_out1,
             keep_ref, send_ref, dog_ref, scr, scr2, sums):
        value_grad, gate_grad = side_grads(y6, vc_ref, gc_ref, scr2, plan)
        terms = side_terms(standard(mid_ref[...].astype(F32))[0].astype(BF16), value_grad, gate_grad, plan)
        mid_grad, gate = mg_ref[...].astype(F32), gate_ref[...]
        lift_grad = (gate * mid_grad).astype(BF16)
        rounded = standard(get_rows(y2, scr, plan.cpd, plan, 0, plan.pos))[0].astype(BF16)
        lifted = nn(nt(eye(plan.c), w_out1[...]).astype(BF16), rounded)
        dog = (lifted * mid_grad * gate * (1.0 - gate)).astype(BF16)
        dog_ref[...] = dog
        normed = standard(z_ref[...].astype(F32))[0].astype(BF16)
        terms += [gg2[...], og2[...], nt(rounded, lift_grad), nt(normed, dog)]
        at = 0
        for part in terms:
            sums[:, at : at + part.shape[1]] = part
            at += part.shape[1]
        half = plan.c // 2
        core = idx[1] & 1
        keep_ref[...] = sums[pl.ds(pl.multiple_of(core * half, 8), half), :]
        send_ref[...] = sums[pl.ds(pl.multiple_of((1 - core) * half, 8), half), :].astype(BF16)

    return body


def last_kernel(plan):
    def body(y8, z_ref, vc_ref, gc_ref, x_ref, scr):
        wide, per = plan.wide, 2 * plan.crow
        value_grad, gate_grad = side_grads(y8, vc_ref, gc_ref, scr, plan)
        normed = standard(z_ref[...].astype(F32))[0].astype(BF16)
        terms = jnp.concatenate(side_terms(normed, value_grad, gate_grad, plan), axis=1)
        totals = []
        for core in range(2):
            total = y8[core, :, plan.pos :].astype(F32)
            for d in range(core + 2, plan.n, 2):
                total = total + y8[d, :, plan.pos :].astype(F32)
            totals.append((total * (1.0 / plan.tokens)).astype(BF16))
        for d in range(plan.n):
            rows = slice(per * (d // 2), per * (d // 2 + 1))
            x_ref[d, :, :wide] = terms[rows, wide * (d % 2) : wide * (d % 2 + 1)].astype(BF16)
            lane = d // plan.cols % 2 * plan.quarter
            x_ref[d, :, wide:] = totals[d % 2][:, lane : lane + plan.quarter]

    return body


def after_last_kernel(plan):
    def body(after, y8, z_ref, mg_ref, dog_ref, vc_ref, gc_ref, vw_ref, gw_ref, w_in1, pg_hbm, scr, flat, pg, sem):
        value_grad, gate_grad = side_grads(y8, vc_ref, gc_ref, scr, plan)
        normed_grad = nn(vw_ref[...], value_grad) + nn(gw_ref[...], gate_grad)
        normed_grad += nn(w_in1[:, 4 * plan.h :], dog_ref[...])
        unit, scale = standard(z_ref[...].astype(F32))
        grad = mg_ref[...].astype(F32) + standard_grad(unit, scale, normed_grad)
        pg[...] = from_lanes(grad.astype(BF16), flat, plan)
        copy = pltpu.make_async_copy(pg, pg_hbm, sem)
        copy.start()
        copy.wait()

    return body


def sum_kernel(plan):
    def body(y_ref, x_ref):
        total = y_ref[0, :, : plan.wide].astype(F32)
        for d in range(1, plan.n):
            total = total + y_ref[d, :, : plan.wide].astype(F32)
        total = (total * (1.0 / plan.tokens)).astype(BF16)
        for d in range(plan.n):
            x_ref[d] = total

    return body


def half_kernel(plan):
    def body(y_ref, half_ref):
        half_ref[...] = y_ref[:, :, plan.wide :]

    return body


def assemble_kernel(plan):
    def body(idx, own, beside, own_far, beside_far, g1_ref, out1_ref, in2_ref, out2_ref, scr):
        h, per = plan.h, 2 * plan.crow
        half = plan.c // 2
        steps = 8 * h // plan.wide
        outs = ((in2_ref, 5 * h), (out2_ref, h), (out1_ref, h), (g1_ref, h))
        row = idx[0] & 1
        for k, pair in enumerate(((own, beside), (own_far, beside_far))):
            for g, ref in ((row, pair[0]), (1 - row, pair[1])):
                for d in range(plan.n):
                    scr[g, per * d : per * (d + 1), :] = ref[d].astype(F32)
            core = idx[1] & 1 if k == 0 else 1 - (idx[1] & 1)
            rows = pl.ds(pl.multiple_of(core * half, 8), half)
            pieces = [
                scr[g, pl.ds(v, half, stride=steps), :] for v in range(steps) for g in range(2)
            ]
            for out_ref, size in outs:
                for i in range(size // LANES):
                    out_ref[rows, i * LANES : (i + 1) * LANES] = pieces.pop(0)

    return body


def end_kernel(plan):
    def body(y_ref, g1_ref, in1_ref):
        wide, per = plan.wide, 2 * plan.crow
        for d in range(plan.n):
            rows = slice(per * (d // 2), per * (d // 2 + 1))
            in1_ref[rows, wide * (d % 2) : wide * (d % 2 + 1)] = y_ref[d].astype(F32)
        in1_ref[:, 2 * wide :] = g1_ref[...]

    return body


def turn_blocks(group, plan):
    count, size = plan.blocks, plan.rt
    lane = iota(group[0].shape, 1)
    group = list(group)
    step = count // 2
    while step:
        low = (lane & (step * size)) == 0
        for a in range(count):
            if a & step == 0:
                x, y = group[a], group[a + step]
                group[a] = jnp.where(low, x, pltpu.roll(y, step * size, 1))
                group[a + step] = jnp.where(low, pltpu.roll(x, LANES - step * size, 1), y)
        step //= 2
    return group


def spread(y_ref, scr, per, plan, steps=1):
    def column(c, carry):
        for g in range(plan.lane_groups):
            for q in range(plan.seconds):
                group = []
                for b in range(plan.blocks):
                    src = (g * plan.blocks + b) * plan.cols + c
                    group.append(y_ref[src, :per, q * LANES : (q + 1) * LANES].astype(F32))
                group = turn_blocks(group, plan)
                for b in range(plan.blocks):
                    row = pl.multiple_of((c * plan.ct + q * plan.blocks + b) * per, per)
                    scr[g, pl.ds(row, per), :] = group[b]
        return carry

    lax.fori_loop(0, plan.cols, column, 0, unroll=plan.cols // steps)


def collect(scr, x_ref, per, plan):
    def column(c, carry):
        for g in range(plan.lane_groups):
            for q in range(plan.seconds):
                group = []
                for b in range(plan.blocks):
                    row = pl.multiple_of((c * plan.ct + q * plan.blocks + b) * per, per)
                    group.append(scr[g, pl.ds(row, per), :])
                group = turn_blocks(group, plan)
                for b in range(plan.blocks):
                    dest = (g * plan.blocks + b) * plan.cols + c
                    x_ref[dest, :per, q * LANES : (q + 1) * LANES] = group[b].astype(BF16)
        return carry

    lax.fori_loop(0, plan.cols, column, 0, unroll=plan.cols)


def pick(scr, row, per, plan):
    parts = [scr[g, pl.ds(row, plan.tokens, stride=per), :] for g in range(plan.lane_groups)]
    return parts[0] if len(parts) == 1 else jnp.concatenate(parts, axis=1)


def place(scr, row, per, value, plan):
    for g in range(plan.lane_groups):
        scr[g, pl.ds(row, plan.tokens, stride=per), :] = value[:, g * LANES : (g + 1) * LANES]


def product_kernel(plan, outgoing):
    cpd = plan.cpd

    def body(y_ref, x_ref, lr_ref, scr, scr_out):
        turn = eye(plan.tokens)
        spread(y_ref, scr, 2 * cpd, plan, 1 if outgoing else 2)
        sides = [pick(scr, row, 2 * cpd, plan).astype(BF16) for row in range(2 * cpd)]
        for row, side in enumerate(sides):
            lr_ref[row] = side
        left, right = sides[:cpd], sides[cpd:]
        if outgoing:
            right = [nt(turn, side).astype(BF16) for side in right]
        for t, tri in enumerate([nn(b, a) if outgoing else nt(b, a) for a, b in zip(left, right)]):
            place(scr_out, t, cpd, tri, plan)
        collect(scr_out, x_ref, cpd, plan)

    return body


def grad_kernel(plan, outgoing):
    cpd = plan.cpd

    def body(*refs):
        if outgoing:
            after, y_ref, lr_ref, keep_ref, other_ref, x_ref, scr, scr_out, scr_sum = refs
        else:
            y_ref, lr_ref, x_ref, scr, scr_out = refs
        turn = eye(plan.tokens)
        spread(y_ref, scr, cpd, plan, 2 if outgoing else 1)
        left = [lr_ref[t] for t in range(cpd)]
        right = [lr_ref[cpd + t] for t in range(cpd)]
        grads = [pick(scr, t, cpd, plan).astype(BF16) for t in range(cpd)]
        if outgoing:
            terms = [nn(b, grad) for b, grad in zip(right, grads)] + [nt(a, grad) for a, grad in zip(left, grads)]
        else:
            turned = [nt(turn, grad).astype(BF16) for grad in grads]
            terms = [nn(grad, b) for b, grad in zip(right, turned)] + [nn(grad, a) for a, grad in zip(left, grads)]
        for row, term in enumerate(terms):
            place(scr_out, row, 2 * cpd, term, plan)
        collect(scr_out, x_ref, 2 * cpd, plan)
        if outgoing:
            half, wide, per = plan.c // 2, plan.wide, 2 * plan.crow
            steps = 8 * plan.h // wide
            total = keep_ref[...] + other_ref[...].astype(F32)
            for v in range(steps):
                for g in range(wide // LANES):
                    at = v * wide + g * LANES
                    scr_sum[g, pl.ds(v, half, stride=steps), :] = total[:, at : at + LANES]
            for d in range(plan.n):
                for g in range(wide // LANES):
                    at = plan.pos + g * LANES
                    x_ref[d, :, at : at + LANES] = scr_sum[g, per * d : per * (d + 1), :].astype(BF16)

    return body


def call(body, name, outs, args, scratch=(), scalars=0, far_in=0, after=0, far_out=()):
    near = pl.BlockSpec(memory_space=pltpu.VMEM)
    far = pl.BlockSpec(memory_space=pltpu.HBM)
    ins = [pl.BlockSpec(memory_space=pltpu.SMEM)] * scalars + [far] * far_in
    args = [
        pltpu.with_memory_space_constraint(a, pltpu.HBM) if scalars <= i < len(ins) else a for i, a in enumerate(args)
    ]
    ins += [pl.BlockSpec(memory_space=pl.ANY)] * after
    return pl.pallas_call(
        body,
        name=name,
        in_specs=ins + [near] * (len(args) - len(ins)),
        out_specs=[far if i in far_out else near for i in range(len(outs))],
        out_shape=[jax.ShapeDtypeStruct(shape, kind) for shape, kind in outs],
        scratch_shapes=[pltpu.VMEM(s, F32) if isinstance(s, tuple) else s for s in scratch],
        compiler_params=pltpu.CompilerParams(vmem_limit_bytes=16 * 1024 * 1024),
    )(*args)


def exchange(x):
    return lax.all_to_all(x, AXES, 0, 0)


def solution(mesh):
    def local(pair, cotangent, token_mask, w_in1, w_out1, w_in2, w_out2):
        rt, ct, c = pair.shape
        h = w_out1.shape[0]
        plan = Plan(mesh, (rt, ct), c, h)
        n, cpd, pos, tokens = plan.n, plan.cpd, plan.pos, plan.tokens
        idx = jnp.stack([lax.axis_index("row"), lax.axis_index("col")]).astype(jnp.int32)
        lanes = (c, pos)
        both = (n, 2 * cpd, pos)
        single = (n, cpd, pos)
        group = plan.lane_groups
        scr1 = (group, tokens * cpd, LANES)
        scr2 = (group, tokens * 2 * cpd, LANES)

        flat = (pos, c)
        dma = pltpu.SemaphoreType.DMA
        halves = (c // 2, 8 * h)
        swap = [(i, i ^ 1) for i in range(plan.cols)]

        lifts = (c, h)
        wide = (2 * h, pos)
        back = (c, 2 * h)
        chip = (plan.wide // LANES, 2 * c, LANES)

        x1, z, mask = call(
            first_kernel(plan), "first", [(both, BF16), (lanes, BF16), ((8, pos), F32)],
            [idx, pair.reshape(flat), token_mask.reshape(1, tokens), w_in1],
            [pltpu.VMEM(flat, BF16), pltpu.VMEM((1, tokens), jnp.int32), pltpu.VMEM((c, 5 * h), BF16), flat, dma((3,))],
            scalars=1, far_in=3,
        )
        y1 = exchange(x1)
        x2, lr1 = call(
            product_kernel(plan, True), "product_out", [(single, BF16), ((2 * cpd, tokens, tokens), BF16)],
            [y1], [scr2, scr1],
        )
        y2 = exchange(x2)
        x3, mid, gate1, vc2, gc2, vw2, gw2 = call(
            middle_kernel(plan), "middle",
            [(both, BF16), (lanes, BF16), (lanes, F32), (wide, BF16), (wide, BF16), (back, BF16), (back, BF16)],
            [z, y2, mask, w_in1, w_out1, w_in2], [(h, pos)],
        )
        y3 = exchange(x3)
        x4, lr2 = call(
            product_kernel(plan, False), "product_in", [(single, BF16), ((2 * cpd, tokens, tokens), BF16)],
            [y3], [scr2, scr1],
        )
        y4 = exchange(x4)
        x5, cot, dog2 = call(
            turn_kernel(plan), "turn", [(single, BF16), (lanes, BF16), (lanes, BF16)],
            [y4, mid, cotangent.reshape(flat), w_in2, w_out2], [(h, pos), flat],
        )
        y5 = exchange(x5)
        (x6,) = call(grad_kernel(plan, False), "grads_in", [(both, BF16)], [y5, lr2], [scr1, scr2])
        y6 = exchange(x6)
        x7, mid_grad = call(
            back_kernel(plan), "back", [(single, BF16), (lanes, BF16)],
            [y6, vc2, gc2, vw2, gw2, dog2, mid, cot, gate1, w_in2, w_out1, y2], [(h, pos), wide],
        )
        y7 = exchange(x7)
        updated, og2, gg2 = call(
            after_turn_kernel(plan), "after_turn", [(flat, BF16), ((h, c), F32), (lifts, F32)],
            [mid_grad, y4, mid, cot, dog2, w_in2, w_out2],
            [(h, pos), flat, pltpu.VMEM(flat, BF16), dma(())], after=1, far_out=(0,),
        )
        keep, send, dog1 = call(
            after_back_kernel(plan), "after_back", [(halves, F32), (halves, BF16), (lanes, BF16)],
            [idx, y6, vc2, gc2, mid, mid_grad, gate1, y2, z, og2, gg2, w_out1],
            [(h, pos), wide, (c, 8 * h)], scalars=1,
        )
        other = lax.ppermute(send, "col", swap)
        vc1, gc1, vw1, gw1 = call(
            before_back_kernel(plan), "before_back1", [(wide, BF16), (wide, BF16), (back, BF16), (back, BF16)],
            [dog1, z, mask, w_in1], after=1,
        )
        (x8,) = call(
            grad_kernel(plan, True), "grads_out", [((n, 2 * cpd, pos + plan.wide), BF16)],
            [vw1, y7, lr1, keep, other], [scr1, scr2, chip], after=1,
        )
        y8 = exchange(x8)
        (x9,) = call(
            last_kernel(plan), "last", [((n, 2 * cpd, plan.wide + plan.quarter), BF16)], [y8, z, vc1, gc1], [wide]
        )
        y9 = exchange(x9)
        (x10,) = call(sum_kernel(plan), "sum", [((n, 2 * cpd, plan.wide), BF16)], [y9])
        y10 = exchange(x10)
        (own,) = call(half_kernel(plan), "half", [((n, 2 * cpd, plan.quarter), BF16)], [y9])
        own_far = lax.ppermute(own, "col", swap)
        beside = lax.ppermute(own, "row", [(i, i ^ 1) for i in range(plan.rows)])
        beside_far = lax.ppermute(beside, "col", swap)
        (pair_grad,) = call(
            after_last_kernel(plan), "after_last", [(flat, BF16)],
            [y9, y8, z, mid_grad, dog1, vc1, gc1, vw1, gw1, w_in1],
            [wide, flat, pltpu.VMEM(flat, BF16), dma(())], after=1, far_out=(0,),
        )
        g1, out1, in2, out2 = call(
            assemble_kernel(plan), "assemble",
            [((c, h), F32), ((h, c), F32), ((c, 5 * h), F32), ((h, c), F32)],
            [idx, own, beside, own_far, beside_far], [chip], scalars=1,
        )
        (in1,) = call(end_kernel(plan), "end", [((c, 5 * h), F32)], [y10, g1])
        return updated.reshape(rt, ct, c), pair_grad.reshape(rt, ct, c), in1, out1, in2, out2

    return jax.shard_map(
        local,
        mesh=mesh,
        in_specs=(P("row", "col", None), P("row", "col", None), P(), P(), P(), P(), P()),
        out_specs=(P("row", "col", None), P("row", "col", None), P(), P(), P(), P()),
        check_vma=False,
    )
```

```python
import jax
import jax.numpy as jnp
from jax import lax
from jax.experimental import pallas as pl
from jax.experimental.pallas import tpu as pltpu
from jax.sharding import PartitionSpec as P

EPSILON = 1e-05
LANES = 128
AXES = ("row", "col")
F32 = jnp.float32
BF16 = jnp.bfloat16


class Plan:
    def __init__(self, mesh, tile, width, hidden):
        self.rows = mesh.shape["row"]
        self.cols = mesh.shape["col"]
        self.n = self.rows * self.cols
        self.rt, self.ct = tile
        self.pos = self.rt * self.ct
        self.tokens = self.rt * self.rows
        self.c = width
        self.h = hidden
        self.cpd = hidden // self.n
        self.crow = width // self.n
        self.blocks = LANES // self.rt
        self.lane_groups = self.tokens // LANES
        self.seconds = self.pos // LANES
        self.wide = 8 * hidden // self.n * (width // 2) // (2 * self.crow)
        self.quarter = self.wide // 2
        assert self.wide == 2 * hidden and self.quarter == LANES
        assert self.cols % 2 == 0 and self.rows % 2 == 0
        assert self.blocks >= 1 and self.cpd == self.crow
        assert self.rt & (self.rt - 1) == 0 and self.rows == self.blocks * self.lane_groups


def nn(a, b):
    return jnp.dot(a, b, preferred_element_type=F32)


def nt(a, b):
    return lax.dot_general(a, b, (((1,), (1,)), ((), ())), preferred_element_type=F32)


def iota(shape, axis):
    return lax.broadcasted_iota(jnp.int32, shape, axis)


def one_hot(cond):
    return jnp.where(cond, 1.0, 0.0).astype(BF16)


def eye(size):
    return one_hot(iota((size, size), 0) == iota((size, size), 1))


def to_lanes(tile_ref, scr, plan):
    scr[...] = tile_ref[...].astype(F32)
    rows = [scr[pl.ds(k, plan.rt, stride=plan.ct), :] for k in range(plan.ct)]
    return nt(eye(plan.c), jnp.concatenate(rows, axis=0).astype(BF16))


def from_lanes(lanes, scr, plan):
    turn = eye(LANES)
    for q in range(plan.seconds):
        block = nt(turn, lanes[:, q * LANES : (q + 1) * LANES])
        for b in range(plan.blocks):
            rows = block[b * plan.rt : (b + 1) * plan.rt, :]
            scr[pl.ds(q * plan.blocks + b, plan.rt, stride=plan.ct), :] = rows
    return scr[...].astype(BF16)


def split_order(plan):
    wide = 2 * plan.h
    row = iota((wide, wide), 0)
    source = iota((wide, wide), 1)
    per = 2 * plan.cpd
    bits = per.bit_length() - 1
    side = (row & (per - 1)) >> (bits - 1)
    channel = (row >> bits) * plan.cpd + (row & (plan.cpd - 1))
    return one_hot(source == side * plan.h + channel)


def sides(w, first, plan):
    h = plan.h
    return jnp.concatenate([w[:, first * h : (first + 1) * h], w[:, (first + 2) * h : (first + 3) * h]], axis=1)


def standard(x):
    centre = jnp.mean(x, axis=0, keepdims=True)
    shifted = x - centre
    spread = jnp.mean(shifted * shifted, axis=0, keepdims=True)
    scale = lax.rsqrt(spread + EPSILON)
    return shifted * scale, scale


def standard_grad(unit, scale, grad):
    flat = jnp.mean(grad, axis=0, keepdims=True)
    along = jnp.mean(grad * unit, axis=0, keepdims=True)
    return scale * (grad - flat - unit * along)


def split_weights(w, perm, plan):
    return nt(perm, sides(w, 0, plan)).astype(BF16), nt(perm, sides(w, 1, plan)).astype(BF16)


def split_projection(normed, value_w, gate_w):
    return nn(value_w, normed), jax.nn.sigmoid(nn(gate_w, normed))


def out_gate(normed, w, plan):
    tail = nt(eye(plan.h), w[:, 4 * plan.h :]).astype(BF16)
    return jax.nn.sigmoid(nn(tail, normed))


def back_coefficients(normed, w, mask, perm, plan):
    value, gate = split_projection(normed, *split_weights(w, perm, plan))
    through = gate * mask
    return through, through * value * (1.0 - gate)


def back_weights(w, perm, plan):
    return nt(sides(w, 0, plan), perm).astype(BF16), nt(sides(w, 1, plan), perm).astype(BF16)


def side_terms(normed, value_grad, gate_grad, perm, plan):
    value_part = nn(nt(normed, value_grad).astype(BF16), perm)
    gate_part = nn(nt(normed, gate_grad).astype(BF16), perm)
    h = plan.h
    return [value_part[:, :h], gate_part[:, :h], value_part[:, h:], gate_part[:, h:]]


def put_rows(dest_ref, value, per, plan, start=0):
    size = value.shape[1]
    for d in range(plan.n):
        dest_ref[d, :, start : start + size] = value[per * d : per * (d + 1), :].astype(dest_ref.dtype)


def get_rows(source_ref, scratch_ref, per, plan, start, size):
    if per % 8 == 0:
        rows = [source_ref[d, :, start : start + size].astype(F32) for d in range(plan.n)]
        return jnp.concatenate(rows, axis=0)
    for d in range(plan.n):
        scratch_ref[per * d : per * (d + 1), :size] = source_ref[d, :, start : start + size].astype(F32)
    return scratch_ref[:, :size]


def first_kernel(plan):
    def body(idx, pair_hbm, tokens_hbm, w_hbm, x_ref, z_ref, mask_ref, perm_ref, pair, tokens, w_in, scr, sems):
        sources = (pair_hbm, tokens_hbm, w_hbm)
        copies = [
            pltpu.make_async_copy(source, dest, sems.at[i])
            for i, (source, dest) in enumerate(zip(sources, (pair, tokens, w_in)))
        ]
        for copy in copies:
            copy.start()
        token = iota((plan.tokens, plan.pos), 0)
        lane = iota((plan.tokens, plan.pos), 1)
        shift = plan.rt.bit_length() - 1
        first = one_hot(token == idx[0] * plan.rt + (lane & (plan.rt - 1)))
        second = one_hot(token == idx[1] * plan.ct + (lane >> shift))
        perm = split_order(plan)
        perm_ref[...] = perm
        for copy in copies:
            copy.wait()
        flags = jnp.broadcast_to(tokens[...].astype(F32), (8, plan.tokens)).astype(BF16)
        mask = nn(flags, first) * nn(flags, second)
        mask_ref[...] = mask
        z = to_lanes(pair, scr, plan)
        z_ref[...] = z.astype(BF16)
        value_w, gate_w = split_weights(w_in[...], perm, plan)
        value, gate = split_projection(standard(z)[0].astype(BF16), value_w, gate_w)
        put_rows(x_ref, gate * value * mask[:1], 2 * plan.cpd, plan)

    return body


def middle_kernel(plan):
    def body(z_ref, y_ref, mask_ref, perm_ref, w_in1, w_out1, w_in2, x_ref, mid_ref, gate_out, vc_ref, gc_ref, vw_ref, gw_ref, scr):
        z = z_ref[...].astype(F32)
        gate = out_gate(standard(z)[0].astype(BF16), w_in1[...], plan)
        gate_out[...] = gate
        tri = get_rows(y_ref, scr, plan.cpd, plan, 0, plan.pos)
        lifted = nn(nt(eye(plan.c), w_out1[...]).astype(BF16), standard(tri)[0].astype(BF16))
        mid = (z + gate * lifted).astype(BF16)
        mid_ref[...] = mid
        normed = standard(mid.astype(F32))[0].astype(BF16)
        value, gate = split_projection(normed, *split_weights(w_in2[...], perm_ref[...], plan))
        through = gate * mask_ref[:1, :]
        part = through * value
        put_rows(x_ref, part, 2 * plan.cpd, plan)
        vc_ref[...] = through.astype(BF16)
        gc_ref[...] = (part * (1.0 - gate)).astype(BF16)
        vw_ref[...], gw_ref[...] = back_weights(w_in2[...], perm_ref[...], plan)

    return body


def turn_kernel(plan):
    def body(y_ref, mid_ref, cot_ref, w_in2, w_out2, x_ref, cot_out, dog_ref, scr, flat):
        cot = to_lanes(cot_ref, flat, plan)
        cot_out[...] = cot.astype(BF16)
        gate = out_gate(standard(mid_ref[...].astype(F32))[0].astype(BF16), w_in2[...], plan)
        lift_grad = (gate * cot).astype(BF16)
        unit, scale = standard(get_rows(y_ref, scr, plan.cpd, plan, 0, plan.pos))
        put_rows(x_ref, standard_grad(unit, scale, nn(w_out2[...], lift_grad)), plan.cpd, plan)
        lifted = nn(nt(eye(plan.c), w_out2[...]).astype(BF16), unit.astype(BF16))
        dog_ref[...] = (lifted * cot * gate * (1.0 - gate)).astype(BF16)

    return body


def after_turn_kernel(plan):
    def body(after, y_ref, mid_ref, cot_ref, dog_ref, w_in2, w_out2, up_hbm, og_ref, gg_ref, scr, flat, up, sem):
        tri = get_rows(y_ref, scr, plan.cpd, plan, 0, plan.pos)
        rounded = standard(tri)[0].astype(BF16)
        lifted = nn(nt(eye(plan.c), w_out2[...]).astype(BF16), rounded)
        mid, cot = mid_ref[...].astype(F32), cot_ref[...].astype(F32)
        normed = standard(mid)[0].astype(BF16)
        gate = out_gate(normed, w_in2[...], plan)
        up[...] = from_lanes((mid + gate * lifted).astype(BF16), flat, plan)
        copy = pltpu.make_async_copy(up, up_hbm, sem)
        copy.start()
        og_ref[...] = nt(rounded, (gate * cot).astype(BF16))
        gg_ref[...] = nt(normed, dog_ref[...])
        copy.wait()

    return body


def before_back_kernel(plan):
    def body(after, source_ref, mask_ref, perm_ref, w_in, vc_ref, gc_ref, vw_ref, gw_ref):
        normed = standard(source_ref[...].astype(F32))[0].astype(BF16)
        value, gate = back_coefficients(normed, w_in[...], mask_ref[:1, :], perm_ref[...], plan)
        vc_ref[...] = value.astype(BF16)
        gc_ref[...] = gate.astype(BF16)
        vw_ref[...], gw_ref[...] = back_weights(w_in[...], perm_ref[...], plan)

    return body


def side_grads(y_ref, vc_ref, gc_ref, scr, plan):
    grad = get_rows(y_ref, scr, 2 * plan.cpd, plan, 0, plan.pos)
    return (grad * vc_ref[...].astype(F32)).astype(BF16), (grad * gc_ref[...].astype(F32)).astype(BF16)


def back_kernel(plan):
    def body(y6, vc_ref, gc_ref, vw_ref, gw_ref, dog_ref, mid_ref, cot_ref, gate_ref, w_in2, w_out1, y2,
             x_ref, mg_ref, scr, scr2):
        value_grad, gate_grad = side_grads(y6, vc_ref, gc_ref, scr2, plan)
        normed_grad = nn(vw_ref[...], value_grad) + nn(gw_ref[...], gate_grad)
        normed_grad += nn(w_in2[:, 4 * plan.h :], dog_ref[...])
        unit, scale = standard(mid_ref[...].astype(F32))
        mid_grad = (cot_ref[...].astype(F32) + standard_grad(unit, scale, normed_grad)).astype(BF16)
        mg_ref[...] = mid_grad
        lift_grad = (gate_ref[...] * mid_grad.astype(F32)).astype(BF16)
        unit, scale = standard(get_rows(y2, scr, plan.cpd, plan, 0, plan.pos))
        put_rows(x_ref, standard_grad(unit, scale, nn(w_out1[...], lift_grad)), plan.cpd, plan)

    return body


def after_back_kernel(plan):
    def body(idx, y6, vc_ref, gc_ref, mid_ref, mg_ref, gate_ref, y2, z_ref, og2, gg2, w_out1, perm_ref,
             keep_ref, send_ref, dog_ref, scr, scr2, sums):
        value_grad, gate_grad = side_grads(y6, vc_ref, gc_ref, scr2, plan)
        terms = side_terms(standard(mid_ref[...].astype(F32))[0].astype(BF16), value_grad, gate_grad, perm_ref[...], plan)
        mid_grad, gate = mg_ref[...].astype(F32), gate_ref[...]
        lift_grad = (gate * mid_grad).astype(BF16)
        rounded = standard(get_rows(y2, scr, plan.cpd, plan, 0, plan.pos))[0].astype(BF16)
        lifted = nn(nt(eye(plan.c), w_out1[...]).astype(BF16), rounded)
        dog = (lifted * mid_grad * gate * (1.0 - gate)).astype(BF16)
        dog_ref[...] = dog
        normed = standard(z_ref[...].astype(F32))[0].astype(BF16)
        terms += [gg2[...], og2[...], nt(rounded, lift_grad), nt(normed, dog)]
        at = 0
        for part in terms:
            sums[:, at : at + part.shape[1]] = part
            at += part.shape[1]
        half = plan.c // 2
        core = idx[1] & 1
        keep_ref[...] = sums[pl.ds(pl.multiple_of(core * half, 8), half), :]
        send_ref[...] = sums[pl.ds(pl.multiple_of((1 - core) * half, 8), half), :].astype(BF16)

    return body


def last_kernel(plan):
    def body(y8, z_ref, vc_ref, gc_ref, perm_ref, x_ref, scr):
        wide, per = plan.wide, 2 * plan.crow
        value_grad, gate_grad = side_grads(y8, vc_ref, gc_ref, scr, plan)
        normed = standard(z_ref[...].astype(F32))[0].astype(BF16)
        terms = jnp.concatenate(side_terms(normed, value_grad, gate_grad, perm_ref[...], plan), axis=1)
        totals = []
        for core in range(2):
            total = y8[core, :, plan.pos :].astype(F32)
            for d in range(core + 2, plan.n, 2):
                total = total + y8[d, :, plan.pos :].astype(F32)
            totals.append((total * (1.0 / plan.tokens)).astype(BF16))
        for d in range(plan.n):
            rows = slice(per * (d // 2), per * (d // 2 + 1))
            x_ref[d, :, :wide] = terms[rows, wide * (d % 2) : wide * (d % 2 + 1)].astype(BF16)
            lane = d // plan.cols % 2 * plan.quarter
            x_ref[d, :, wide:] = totals[d % 2][:, lane : lane + plan.quarter]

    return body


def after_last_kernel(plan):
    def body(after, y8, z_ref, mg_ref, dog_ref, vc_ref, gc_ref, vw_ref, gw_ref, w_in1, pg_hbm, scr, flat, pg, sem):
        value_grad, gate_grad = side_grads(y8, vc_ref, gc_ref, scr, plan)
        normed_grad = nn(vw_ref[...], value_grad) + nn(gw_ref[...], gate_grad)
        normed_grad += nn(w_in1[:, 4 * plan.h :], dog_ref[...])
        unit, scale = standard(z_ref[...].astype(F32))
        grad = mg_ref[...].astype(F32) + standard_grad(unit, scale, normed_grad)
        pg[...] = from_lanes(grad.astype(BF16), flat, plan)
        copy = pltpu.make_async_copy(pg, pg_hbm, sem)
        copy.start()
        copy.wait()

    return body


def sum_kernel(plan):
    def body(y_ref, x_ref):
        total = y_ref[0, :, : plan.wide].astype(F32)
        for d in range(1, plan.n):
            total = total + y_ref[d, :, : plan.wide].astype(F32)
        total = (total * (1.0 / plan.tokens)).astype(BF16)
        for d in range(plan.n):
            x_ref[d] = total

    return body


def half_kernel(plan):
    def body(y_ref, half_ref):
        half_ref[...] = y_ref[:, :, plan.wide :]

    return body


def assemble_kernel(plan):
    def body(idx, own, beside, own_far, beside_far, g1_ref, out1_ref, in2_ref, out2_ref, scr):
        h, per = plan.h, 2 * plan.crow
        half = plan.c // 2
        steps = 8 * h // plan.wide
        outs = ((in2_ref, 5 * h), (out2_ref, h), (out1_ref, h), (g1_ref, h))
        row = idx[0] & 1
        for k, pair in enumerate(((own, beside), (own_far, beside_far))):
            for g, ref in ((row, pair[0]), (1 - row, pair[1])):
                for d in range(plan.n):
                    scr[g, per * d : per * (d + 1), :] = ref[d].astype(F32)
            core = idx[1] & 1 if k == 0 else 1 - (idx[1] & 1)
            rows = pl.ds(pl.multiple_of(core * half, 8), half)
            pieces = [
                scr[g, pl.ds(v, half, stride=steps), :] for v in range(steps) for g in range(2)
            ]
            for out_ref, size in outs:
                for i in range(size // LANES):
                    out_ref[rows, i * LANES : (i + 1) * LANES] = pieces.pop(0)

    return body


def end_kernel(plan):
    def body(y_ref, g1_ref, in1_ref):
        wide, per = plan.wide, 2 * plan.crow
        for d in range(plan.n):
            rows = slice(per * (d // 2), per * (d // 2 + 1))
            in1_ref[rows, wide * (d % 2) : wide * (d % 2 + 1)] = y_ref[d].astype(F32)
        in1_ref[:, 2 * wide :] = g1_ref[...]

    return body


def turn_blocks(group, plan):
    count, size = plan.blocks, plan.rt
    lane = iota(group[0].shape, 1)
    group = list(group)
    step = count // 2
    while step:
        low = (lane & (step * size)) == 0
        for a in range(count):
            if a & step == 0:
                x, y = group[a], group[a + step]
                group[a] = jnp.where(low, x, pltpu.roll(y, step * size, 1))
                group[a + step] = jnp.where(low, pltpu.roll(x, LANES - step * size, 1), y)
        step //= 2
    return group


def spread(y_ref, scr, per, plan, steps=1):
    def column(c, carry):
        for g in range(plan.lane_groups):
            for q in range(plan.seconds):
                group = []
                for b in range(plan.blocks):
                    src = (g * plan.blocks + b) * plan.cols + c
                    group.append(y_ref[src, :per, q * LANES : (q + 1) * LANES].astype(F32))
                group = turn_blocks(group, plan)
                for b in range(plan.blocks):
                    row = pl.multiple_of((c * plan.ct + q * plan.blocks + b) * per, per)
                    scr[g, pl.ds(row, per), :] = group[b]
        return carry

    lax.fori_loop(0, plan.cols, column, 0, unroll=plan.cols // steps)


def collect(scr, x_ref, per, plan):
    def column(c, carry):
        for g in range(plan.lane_groups):
            for q in range(plan.seconds):
                group = []
                for b in range(plan.blocks):
                    row = pl.multiple_of((c * plan.ct + q * plan.blocks + b) * per, per)
                    group.append(scr[g, pl.ds(row, per), :])
                group = turn_blocks(group, plan)
                for b in range(plan.blocks):
                    dest = (g * plan.blocks + b) * plan.cols + c
                    x_ref[dest, :per, q * LANES : (q + 1) * LANES] = group[b].astype(BF16)
        return carry

    lax.fori_loop(0, plan.cols, column, 0, unroll=plan.cols)


def pick(scr, row, per, plan):
    parts = [scr[g, pl.ds(row, plan.tokens, stride=per), :] for g in range(plan.lane_groups)]
    return parts[0] if len(parts) == 1 else jnp.concatenate(parts, axis=1)


def place(scr, row, per, value, plan):
    for g in range(plan.lane_groups):
        scr[g, pl.ds(row, plan.tokens, stride=per), :] = value[:, g * LANES : (g + 1) * LANES]


def product_kernel(plan, outgoing):
    cpd = plan.cpd

    def body(y_ref, x_ref, lr_ref, scr, scr_out):
        turn = eye(plan.tokens)
        spread(y_ref, scr, 2 * cpd, plan, 1 if outgoing else 2)
        sides = [pick(scr, row, 2 * cpd, plan).astype(BF16) for row in range(2 * cpd)]
        for row, side in enumerate(sides):
            lr_ref[row] = side
        left, right = sides[:cpd], sides[cpd:]
        if outgoing:
            right = [nt(turn, side).astype(BF16) for side in right]
        for t, tri in enumerate([nn(b, a) if outgoing else nt(b, a) for a, b in zip(left, right)]):
            place(scr_out, t, cpd, tri, plan)
        collect(scr_out, x_ref, cpd, plan)

    return body


def grad_kernel(plan, outgoing):
    cpd = plan.cpd

    def body(*refs):
        if outgoing:
            after, y_ref, lr_ref, keep_ref, other_ref, x_ref, scr, scr_out, scr_sum = refs
        else:
            y_ref, lr_ref, x_ref, scr, scr_out = refs
        turn = eye(plan.tokens)
        spread(y_ref, scr, cpd, plan, 2 if outgoing else 1)
        left = [lr_ref[t] for t in range(cpd)]
        right = [lr_ref[cpd + t] for t in range(cpd)]
        grads = [pick(scr, t, cpd, plan).astype(BF16) for t in range(cpd)]
        if outgoing:
            terms = [nn(b, grad) for b, grad in zip(right, grads)] + [nt(a, grad) for a, grad in zip(left, grads)]
        else:
            turned = [nt(turn, grad).astype(BF16) for grad in grads]
            terms = [nn(grad, b) for b, grad in zip(right, turned)] + [nn(grad, a) for a, grad in zip(left, grads)]
        for row, term in enumerate(terms):
            place(scr_out, row, 2 * cpd, term, plan)
        collect(scr_out, x_ref, 2 * cpd, plan)
        if outgoing:
            half, wide, per = plan.c // 2, plan.wide, 2 * plan.crow
            steps = 8 * plan.h // wide
            total = keep_ref[...] + other_ref[...].astype(F32)
            for v in range(steps):
                for g in range(wide // LANES):
                    at = v * wide + g * LANES
                    scr_sum[g, pl.ds(v, half, stride=steps), :] = total[:, at : at + LANES]
            for d in range(plan.n):
                for g in range(wide // LANES):
                    at = plan.pos + g * LANES
                    x_ref[d, :, at : at + LANES] = scr_sum[g, per * d : per * (d + 1), :].astype(BF16)

    return body


def call(body, name, outs, args, scratch=(), scalars=0, far_in=0, after=0, far_out=()):
    near = pl.BlockSpec(memory_space=pltpu.VMEM)
    far = pl.BlockSpec(memory_space=pltpu.HBM)
    ins = [pl.BlockSpec(memory_space=pltpu.SMEM)] * scalars + [far] * far_in
    args = [
        pltpu.with_memory_space_constraint(a, pltpu.HBM) if scalars <= i < len(ins) else a for i, a in enumerate(args)
    ]
    ins += [pl.BlockSpec(memory_space=pl.ANY)] * after
    return pl.pallas_call(
        body,
        name=name,
        in_specs=ins + [near] * (len(args) - len(ins)),
        out_specs=[far if i in far_out else near for i in range(len(outs))],
        out_shape=[jax.ShapeDtypeStruct(shape, kind) for shape, kind in outs],
        scratch_shapes=[pltpu.VMEM(s, F32) if isinstance(s, tuple) else s for s in scratch],
        compiler_params=pltpu.CompilerParams(vmem_limit_bytes=16 * 1024 * 1024),
    )(*args)


def exchange(x):
    return lax.all_to_all(x, AXES, 0, 0)


def solution(mesh):
    def local(pair, cotangent, token_mask, w_in1, w_out1, w_in2, w_out2):
        rt, ct, c = pair.shape
        h = w_out1.shape[0]
        plan = Plan(mesh, (rt, ct), c, h)
        n, cpd, pos, tokens = plan.n, plan.cpd, plan.pos, plan.tokens
        idx = jnp.stack([lax.axis_index("row"), lax.axis_index("col")]).astype(jnp.int32)
        lanes = (c, pos)
        both = (n, 2 * cpd, pos)
        single = (n, cpd, pos)
        group = plan.lane_groups
        scr1 = (group, tokens * cpd, LANES)
        scr2 = (group, tokens * 2 * cpd, LANES)

        flat = (pos, c)
        dma = pltpu.SemaphoreType.DMA
        halves = (c // 2, 8 * h)
        swap = [(i, i ^ 1) for i in range(plan.cols)]

        lifts = (c, h)
        wide = (2 * h, pos)
        back = (c, 2 * h)
        chip = (plan.wide // LANES, 2 * c, LANES)

        x1, z, mask, perm = call(
            first_kernel(plan), "first",
            [(both, BF16), (lanes, BF16), ((8, pos), F32), ((2 * h, 2 * h), BF16)],
            [idx, pair.reshape(flat), token_mask.reshape(1, tokens), w_in1],
            [pltpu.VMEM(flat, BF16), pltpu.VMEM((1, tokens), jnp.int32), pltpu.VMEM((c, 5 * h), BF16), flat, dma((3,))],
            scalars=1, far_in=3,
        )
        y1 = exchange(x1)
        x2, lr1 = call(
            product_kernel(plan, True), "product_out", [(single, BF16), ((2 * cpd, tokens, tokens), BF16)],
            [y1], [scr2, scr1],
        )
        y2 = exchange(x2)
        x3, mid, gate1, vc2, gc2, vw2, gw2 = call(
            middle_kernel(plan), "middle",
            [(both, BF16), (lanes, BF16), (lanes, F32), (wide, BF16), (wide, BF16), (back, BF16), (back, BF16)],
            [z, y2, mask, perm, w_in1, w_out1, w_in2], [(h, pos)],
        )
        y3 = exchange(x3)
        x4, lr2 = call(
            product_kernel(plan, False), "product_in", [(single, BF16), ((2 * cpd, tokens, tokens), BF16)],
            [y3], [scr2, scr1],
        )
        y4 = exchange(x4)
        x5, cot, dog2 = call(
            turn_kernel(plan), "turn", [(single, BF16), (lanes, BF16), (lanes, BF16)],
            [y4, mid, cotangent.reshape(flat), w_in2, w_out2], [(h, pos), flat],
        )
        y5 = exchange(x5)
        (x6,) = call(grad_kernel(plan, False), "grads_in", [(both, BF16)], [y5, lr2], [scr1, scr2])
        y6 = exchange(x6)
        x7, mid_grad = call(
            back_kernel(plan), "back", [(single, BF16), (lanes, BF16)],
            [y6, vc2, gc2, vw2, gw2, dog2, mid, cot, gate1, w_in2, w_out1, y2], [(h, pos), wide],
        )
        y7 = exchange(x7)
        updated, og2, gg2 = call(
            after_turn_kernel(plan), "after_turn", [(flat, BF16), ((h, c), F32), (lifts, F32)],
            [mid_grad, y4, mid, cot, dog2, w_in2, w_out2],
            [(h, pos), flat, pltpu.VMEM(flat, BF16), dma(())], after=1, far_out=(0,),
        )
        keep, send, dog1 = call(
            after_back_kernel(plan), "after_back", [(halves, F32), (halves, BF16), (lanes, BF16)],
            [idx, y6, vc2, gc2, mid, mid_grad, gate1, y2, z, og2, gg2, w_out1, perm],
            [(h, pos), wide, (c, 8 * h)], scalars=1,
        )
        other = lax.ppermute(send, "col", swap)
        vc1, gc1, vw1, gw1 = call(
            before_back_kernel(plan), "before_back1", [(wide, BF16), (wide, BF16), (back, BF16), (back, BF16)],
            [dog1, z, mask, perm, w_in1], after=1,
        )
        (x8,) = call(
            grad_kernel(plan, True), "grads_out", [((n, 2 * cpd, pos + plan.wide), BF16)],
            [vw1, y7, lr1, keep, other], [scr1, scr2, chip], after=1,
        )
        y8 = exchange(x8)
        (x9,) = call(
            last_kernel(plan), "last", [((n, 2 * cpd, plan.wide + plan.quarter), BF16)], [y8, z, vc1, gc1, perm], [wide]
        )
        y9 = exchange(x9)
        (x10,) = call(sum_kernel(plan), "sum", [((n, 2 * cpd, plan.wide), BF16)], [y9])
        y10 = exchange(x10)
        (own,) = call(half_kernel(plan), "half", [((n, 2 * cpd, plan.quarter), BF16)], [y9])
        own_far = lax.ppermute(own, "col", swap)
        beside = lax.ppermute(own, "row", [(i, i ^ 1) for i in range(plan.rows)])
        beside_far = lax.ppermute(beside, "col", swap)
        (pair_grad,) = call(
            after_last_kernel(plan), "after_last", [(flat, BF16)],
            [y9, y8, z, mid_grad, dog1, vc1, gc1, vw1, gw1, w_in1],
            [wide, flat, pltpu.VMEM(flat, BF16), dma(())], after=1, far_out=(0,),
        )
        g1, out1, in2, out2 = call(
            assemble_kernel(plan), "assemble",
            [((c, h), F32), ((h, c), F32), ((c, 5 * h), F32), ((h, c), F32)],
            [idx, own, beside, own_far, beside_far], [chip], scalars=1,
        )
        (in1,) = call(end_kernel(plan), "end", [((c, 5 * h), F32)], [y10, g1])
        return updated.reshape(rt, ct, c), pair_grad.reshape(rt, ct, c), in1, out1, in2, out2

    return jax.shard_map(
        local,
        mesh=mesh,
        in_specs=(P("row", "col", None), P("row", "col", None), P(), P(), P(), P(), P()),
        out_specs=(P("row", "col", None), P("row", "col", None), P(), P(), P(), P()),
        check_vma=False,
    )
```
